512 devices in a mesh: tile: 128 (over y, z, core), col: 4 (over x).
Axes of the slice: x: 4, y: 8, z: 8, core: 2. Of those that a mesh axis runs over, the one named last changes fastest.
Arguments:
- positions: float32 [3, 65536], P(None, 'tile'), may hold values from 0 to 10240, as said below
- trial_block: float32 [3, 16, 65536], P(None, None, 'tile')
- pair_tiles: int32 [2, 128, 4, 8], P(None, 'tile'), may hold values from 0 to 511, as said below
- pair_count: int32 [128, 4], P('tile'), may hold values from 0 to 8, as said below
Outputs:
- next_block: float32 [3, 16, 65536], P(None, None, 'tile')
- rayleigh: float32 [16, 16], replicated
- correlation_norm: float32 [16, 16], replicated
- residual_norms: float32 [16], replicated
The draws below stay inside these ranges and needn't reach their ends.
Inputs may be any that keep to these rules, and one draw needn't show every extreme that they name: `positions`: tiles follow one another along the first component, in order of their numbers. `pair_tiles`: entry 1 lies between the row tile and two tiles past it, never below it, within the tiles of the same index along tile or of the next one. Each unordered pair of tiles is listed at most once among live slots; every pair of beads closer than 15 is covered by a live slot. Slots at or past the count hold valid numbers too. `pair_count`: for every index along tile but the last, one of its 4 devices along col has all 8 slots live.
All inputs are finite; a program needn't handle non-finite values.
Results may differ from the reference program's by a relative error of at most 0.0003.
Values sent between devices are 32-bit elements; how exact they have to be, the bound alone decides.
A program may use at most 64 MiB of HBM per device.

```python
import jax
import jax.numpy as jnp
from jax import lax

TILE_B = 128
COLS = 16
R_DEV = 4
P_DEV = 8
ITERS = 2
TILES = 512
BEADS = 65536
N_TILE = 128
N_COL = 4


def tile_layout(key):
    thick = jax.random.randint(jax.random.fold_in(key, 7), (TILES,), 10, 21).astype(jnp.int32)
    start = (jnp.cumsum(thick) - thick).astype(jnp.int32)
    return (thick, start)


def pair_layout(key):
    thick, start = tile_layout(key)
    finish = start + thick
    tile_range = jnp.arange(TILES, dtype=jnp.int32)
    reach = jnp.arange(3, dtype=jnp.int32)
    partner = tile_range[:, None] + reach[None, :]
    safe_partner = jnp.minimum(partner, TILES - 1)
    spacing = start[safe_partner] - finish[:, None]
    linked = (reach[None, :] == 0) | (partner < TILES) & (spacing < 15)
    linked_group = linked.reshape(N_TILE, R_DEV * 3)
    cand_range = jnp.arange(R_DEV * 3, dtype=jnp.int32)
    score = jnp.where(linked_group, cand_range[None, :], cand_range[None, :] + 3 * R_DEV)
    order = jnp.argsort(score, axis=1, stable=True).astype(jnp.int32)
    length = jnp.sum(linked_group.astype(jnp.int32), axis=1)
    heavy = jax.random.randint(jax.random.fold_in(key, 13), (N_TILE,), 0, N_COL).astype(jnp.int32)
    slot_range = jnp.arange(P_DEV, dtype=jnp.int32)
    dev_range = jnp.arange(N_COL, dtype=jnp.int32)
    rank = jnp.where(dev_range[None, :] < heavy[:, None], dev_range[None, :], dev_range[None, :] - 1)
    is_heavy = dev_range[None, :] == heavy[:, None]
    item = jnp.where(is_heavy[:, :, None], slot_range[None, None, :], P_DEV + slot_range[None, None, :] * (N_COL - 1) + rank[:, :, None])
    live = item < length[:, None, None]
    count = jnp.sum(live.astype(jnp.int32), axis=2)
    item_safe = jnp.minimum(item, 3 * R_DEV - 1)
    order_wide = jnp.broadcast_to(order[:, None, :], (N_TILE, N_COL, 3 * R_DEV))
    chosen = jnp.take_along_axis(order_wide, item_safe, axis=2)
    row_local = chosen // 3
    group_first = jnp.arange(N_TILE, dtype=jnp.int32)[:, None, None] * R_DEV
    col_global = jnp.minimum(group_first + row_local + chosen % 3, TILES - 1)
    return (jnp.stack([row_local, col_global]).astype(jnp.int32), count.astype(jnp.int32))


def draw_positions(key, part):
    thick, start = tile_layout(key)
    key_along, key_across = jax.random.split(jax.random.fold_in(key, 11))
    along = jax.random.uniform(key_along, (TILES, TILE_B), jnp.float32) * thick[:, None].astype(jnp.float32)
    along = along + start[:, None].astype(jnp.float32)
    across = jax.random.uniform(key_across, (2, TILES, TILE_B), jnp.float32, 0.0, 22.0)
    return jnp.concatenate([along[None], across], axis=0).reshape(3, BEADS)


def draw_trial_block(key, part):
    key_base, key_scale = jax.random.split(key, 2)
    values_base = jax.random.normal(key_base, (3, COLS, BEADS), jnp.float32)
    column_scale = 0.3 * jnp.exp(jax.random.uniform(key_scale, (COLS,), jnp.float32, 0.0, jnp.log(10.0)))
    position = jnp.arange(BEADS, dtype=jnp.float32) / BEADS
    growth = 1.0 + 2.0 * position
    return values_base * column_scale[None, :, None] * growth[None, None, :]


def draw_pair_tiles(key, part):
    lists, count = pair_layout(key)
    return lists


def draw_pair_count(key, part):
    lists, count = pair_layout(key)
    return count


def setup_inputs(seed: int = 0) -> dict:
    key_of = jax.random.split(jax.random.key(seed), 5)
    positions = draw_positions(jax.random.fold_in(key_of[4], 71), 0)
    trial_block = draw_trial_block(jax.random.fold_in(key_of[4], 71), 0)
    pair_tiles = draw_pair_tiles(jax.random.fold_in(key_of[4], 71), 0)
    pair_count = draw_pair_count(jax.random.fold_in(key_of[4], 71), 0)
    return dict(positions=positions, trial_block=trial_block, pair_tiles=pair_tiles, pair_count=pair_count)


spring_scale = 1.0 / 64.0
cutoff_sq = 225.0
step_size = 0.2
highest = lax.Precision.HIGHEST

def pair_terms(pos_rows, pos_cols, vec_rows, vec_cols):
    offset = pos_cols[:, :, None, :] - pos_rows[:, :, :, None]
    dist_sq = jnp.sum(offset * offset, axis=0)
    falloff = jnp.where(dist_sq < cutoff_sq, (1.0 - dist_sq / cutoff_sq) ** 2, 0.0)
    weight = spring_scale * falloff / jnp.maximum(dist_sq, 1.0)
    spring = weight[None, None] * offset[:, None] * offset[None, :]
    row_diag = jnp.sum(spring, axis=-1)
    col_diag = jnp.sum(spring, axis=-2)
    row_term = jnp.einsum('cdpa,dkpa->pcka', row_diag, vec_rows, precision=highest) - jnp.einsum('cdpab,dkpb->pcka', spring, vec_cols, precision=highest)
    col_term = jnp.einsum('cdpb,dkpb->pckb', col_diag, vec_cols, precision=highest) - jnp.einsum('cdpab,dkpa->pckb', spring, vec_rows, precision=highest)
    return (row_term, col_term)

def project_out(correlation, gram_sum):
    factor = jnp.linalg.cholesky(correlation)
    middle = lax.linalg.triangular_solve(factor, gram_sum, left_side=True, lower=True)
    return lax.linalg.triangular_solve(factor, middle, left_side=True, lower=True, transpose_a=True)

def reference(positions, trial_block, pair_tiles, pair_count):
    tile_count = N_TILE * R_DEV
    pos_tiles = positions.reshape(3, tile_count, TILE_B)
    slot_range = jnp.arange(P_DEV, dtype=jnp.int32)
    is_live = (slot_range[None, None, :] < pair_count[:, :, None]).astype(jnp.float32)
    row_ids = (jnp.arange(N_TILE, dtype=jnp.int32)[:, None, None] * R_DEV + pair_tiles[0]).astype(jnp.int32)
    col_ids = pair_tiles[1].astype(jnp.int32)
    off_diag = is_live * (col_ids != row_ids).astype(jnp.float32)
    groups = (row_ids.reshape(-1, 8), col_ids.reshape(-1, 8), is_live.reshape(-1, 8), off_diag.reshape(-1, 8))
    current = trial_block
    for iteration in range(ITERS):
        vec_tiles = current.reshape(3, COLS, tile_count, TILE_B)

        def add_group(running, group_now):
            rows_now, cols_now, live_now, far_now = group_now
            row_term, col_term = pair_terms(jnp.take(pos_tiles, rows_now, axis=1), jnp.take(pos_tiles, cols_now, axis=1), jnp.take(vec_tiles, rows_now, axis=2), jnp.take(vec_tiles, cols_now, axis=2))
            row_term = row_term * live_now[:, None, None, None]
            col_term = col_term * far_now[:, None, None, None]
            running = running.at[:, :, rows_now, :].add(jnp.transpose(row_term, (1, 2, 0, 3)))
            running = running.at[:, :, cols_now, :].add(jnp.transpose(col_term, (1, 2, 0, 3)))
            return (running, None)
        product, _ = lax.scan(add_group, jnp.zeros((3, COLS, tile_count, TILE_B), jnp.float32), groups)
        product = product.reshape(3, COLS, BEADS)
        gram_sum = jnp.einsum('dkb,dlb->kl', current, product, precision=highest)
        correlation = jnp.einsum('dkb,dlb->kl', current, current, precision=highest)
        coefficients = project_out(correlation, gram_sum)
        residual = product - jnp.einsum('jk,djb->dkb', coefficients, current, precision=highest)
        current = current - step_size * residual
    bead_scale = 1.0 / (3.0 * BEADS)
    resid_norms = jnp.sum(residual * residual, axis=(0, 2))
    return (current, gram_sum * bead_scale, correlation * bead_scale, resid_norms * bead_scale)
```

```python
import functools

import jax
import jax.numpy as jnp
from jax import lax
from jax.experimental import pallas as pl
from jax.experimental.pallas import tpu as pltpu
from jax.sharding import Mesh
from jax.sharding import PartitionSpec as P

TILE = ("ty", "tz", "core")
MESH = pl.DeviceIdType.MESH
F32 = jnp.float32
BF16 = jnp.bfloat16
HIGHEST = lax.Precision.HIGHEST

STEP = 0.2
MATS = ((0, 0), (0, 1), (0, 2), (1, 1), (1, 2), (2, 2))
MAT_OF = {(0, 0): 0, (0, 1): 1, (1, 0): 1, (0, 2): 2, (2, 0): 2, (1, 1): 3, (1, 2): 4, (2, 1): 4, (2, 2): 5}


def iota(shape, axis):
    return lax.broadcasted_iota(jnp.int32, shape, axis)


def split(x):
    hi = x.astype(BF16)
    return hi, (x - hi.astype(F32)).astype(BF16)


def mm(a, b):
    return lax.dot_general(a, b, (((1,), (0,)), ((), ())), preferred_element_type=F32)


def solve(z):
    m = z[:, 0:16]
    lane = iota((32, 16), 1)
    for j in range(16):
        col = m[:, j : j + 1]
        inv = 1.0 / m[j : j + 1, j : j + 1]
        row = m[j : j + 1, :] * inv
        m = jnp.where(lane == j, col * inv, m - col * row)
    return m[16:32, :]


def kernel(
    ny, nz, scale,
    x_ref, pos_ref, pairs_ref, count_ref,
    next_ref, ray_ref, corr_ref, norm_ref,
    xg, x1, pg, shi, slo, lw, dacc, pay, ra, rb, rc, tot,
    halo_send, halo_recv, p_send, p_recv, a_send, a_recv, b_send, b_recv, c_send, c_recv, t_send, t_recv,
):
    ty, tz, core, col = (lax.axis_index(n) for n in ("ty", "tz", "core", "col"))
    tiles = ny * nz * 2
    t = (ty * nz + tz) * 2 + core
    low = col < 2

    def at_tile(index, c):
        return (lax.div(index, 2 * nz), lax.rem(lax.div(index, 2), nz), lax.rem(index, 2), c)

    after, before = lax.rem(t + 1, tiles), lax.rem(t + tiles - 1, tiles)
    across = jnp.where(low, before, after)
    across_cols = (jnp.where(low, 2, 0), jnp.where(low, 3, 1))

    barrier = pltpu.get_barrier_semaphore()

    def greet(where):
        pl.semaphore_signal(barrier, inc=1, device_id=where, device_id_type=MESH)

    @pl.when(core == 1)
    def _():
        for o in range(1, ny):
            greet((lax.rem(ty + o, ny), tz, core, col))
        for o in range(1, nz):
            greet((ty, lax.rem(tz + o, nz), core, col))

    for c in across_cols:
        greet(at_tile(across, c))
    greet(at_tile(after, col))
    greet(at_tile(before, col))
    for o in range(1, 4):
        greet((ty, tz, core, lax.rem(col + o, 4)))
        greet((ty, tz, 1 - core, lax.rem(col + o, 4)))
    greet((ty, tz, 1 - core, col))

    lane = iota((1, 128), 1)
    rows, cols = pairs_ref[0], pairs_ref[1]
    slot_col = iota((4, 8), 0)
    counts = jnp.zeros((4, 8), jnp.int32)
    for c in range(4):
        counts = jnp.where(slot_col == c, count_ref[0, c], counts)
    live = jnp.where(iota((4, 8), 1) < counts, 1.0, 0.0).astype(F32)
    reach = cols - t * 4 - rows
    for r in range(4):
        xg[2 + r, 0:48, :] = x_ref[:, r * 128 : (r + 1) * 128]
        xg[2 + r, 48:56, :] = jnp.zeros((8, 128), F32)
        xg[2 + r, 48:51, :] = pos_ref[:, r * 128 : (r + 1) * 128]
        listed = jnp.zeros((1, 128), F32)
        for k in range(3):
            here = jnp.where((rows == r) & (reach == k), live, 0.0)
            total = jnp.sum(jnp.sum(here, axis=1, keepdims=True), axis=0, keepdims=True)
            listed = jnp.where(lane == k, total, listed)
        xg[2 + r, 51:52, :] = listed

    dacc[...] = jnp.zeros_like(dacc)
    own = 2 + col

    def spring_block(q, slot):
        mine = [xg[own, 48 + d : 49 + d, :] for d in range(3)]
        listed = xg[jnp.minimum(slot, own), 51:52, :]
        times = jnp.sum(jnp.where(lane == jnp.abs(slot - own), listed, 0.0), axis=1, keepdims=True)
        times = times * (1.0 / 64.0)
        near = jnp.transpose(xg[slot, 48:56, :])
        sums = [dacc[m] for m in range(6)]
        for ch in range(4):
            part = near[ch * 32 : (ch + 1) * 32]
            off = [part[:, d : d + 1] - mine[d] for d in range(3)]
            dist = off[0] * off[0] + off[1] * off[1] + off[2] * off[2]
            fall = 1.0 - dist * (1.0 / 225.0)
            weight = jnp.where(dist < 225.0, fall * fall, 0.0) * times / jnp.maximum(dist, 1.0)
            by = [weight * o for o in off]
            at = pl.ds(pl.multiple_of(q * 128 + ch * 32, 32), 32)
            for m, (c, d) in enumerate(MATS):
                s = by[c] * off[d]
                hi, lo = split(s)
                shi[at, m * 128 : (m + 1) * 128] = hi
                slo[at, m * 128 : (m + 1) * 128] = lo
                sums[m] = sums[m] + ((s[0:8] + s[8:16]) + (s[16:24] + s[24:32]))
        for m in range(6):
            dacc[m] = sums[m]

    first = jnp.where(low, 2, 3)
    late = (
        jnp.where(col == 0, 0, jnp.where(col == 1, 1, jnp.where(col == 2, 2, 6))),
        jnp.where(col == 0, 1, jnp.where(col == 1, 5, jnp.where(col == 2, 6, 7))),
    )
    slots = (first, first + 1, first + 2) + late

    pl.semaphore_wait(barrier, 11 + core * (ny + nz - 2))
    from_slot, to_slot = jnp.where(low, 4, 2), jnp.where(low, 0, 6)
    halo = pltpu.make_async_remote_copy(
        src_ref=xg.at[pl.ds(from_slot, 2)],
        dst_ref=xg.at[pl.ds(to_slot, 2)],
        send_sem=halo_send,
        recv_sem=halo_recv,
        device_id=at_tile(jnp.where(low, after, before), col),
        device_id_type=MESH,
    )
    halo.start()

    def near_vectors(source, q):
        hi, lo = split(source[slots[q], 0:48, :])
        lw[0:48, q * 128 : (q + 1) * 128] = hi
        lw[48:96, q * 128 : (q + 1) * 128] = lo

    def near_sum(start, stop):
        a, b = start * 128, stop * 128
        both = mm(lw[:, a:b], shi[a:b, :])
        return both[0:48] + both[48:96] + mm(lw[0:48, a:b], slo[a:b, :])

    def first_blocks(q, carry):
        spring_block(q, first + q)
        return carry

    lax.fori_loop(0, 3, first_blocks, 0)
    for q in range(3):
        near_vectors(xg, q)
    gathered = near_sum(0, 3)
    halo.wait_recv()

    def late_blocks(q, carry):
        spring_block(3 + q, jnp.where(q == 0, late[0], late[1]))
        return carry

    lax.fori_loop(0, 2, late_blocks, 0)
    for q in range(3, 5):
        near_vectors(xg, q)
    gathered = gathered + near_sum(3, 5)
    diag = [jnp.sum(dacc[m], axis=0, keepdims=True) for m in range(6)]

    def finish_product(gathered, source):
        here = [source[own, d * 16 : (d + 1) * 16, :] for d in range(3)]
        out = []
        for c in range(3):
            acc = None
            for d in range(3):
                m = MAT_OF[(c, d)]
                term = diag[m] * here[d] - gathered[d * 16 : (d + 1) * 16, m * 128 : (m + 1) * 128]
                acc = term if acc is None else acc + term
            out.append(acc)
        return here, out

    def exchange(it, here, product, halo_too):
        for d in range(3):
            pg[it, own, d * 16 : (d + 1) * 16, :] = product[d]
        both = jnp.concatenate([jnp.concatenate(here, axis=1), jnp.concatenate(product, axis=1)], axis=0)
        z = lax.dot_general(both, both, (((1,), (1,)), ((), ())), precision=HIGHEST, preferred_element_type=F32)
        for g in range(4):
            pay[it, :, g * 32 : (g + 1) * 32] = z[g * 8 : (g + 1) * 8, :]
        line = col * 2 + core

        def to_line(x):
            return pltpu.make_async_remote_copy(
                src_ref=pay.at[it], dst_ref=ra.at[it, line], send_sem=a_send.at[it, x], recv_sem=a_recv.at[it, line],
                device_id=(ty, tz, 1, x), device_id_type=MESH,
            )

        for x in range(4):
            @pl.when(jnp.logical_or(core == 0, col != x))
            def _():
                to_line(x).start()

        sent = []

        def send_product(n, slot, where):
            copy = pltpu.make_async_remote_copy(
                src_ref=pg.at[it, own], dst_ref=pg.at[it, slot], send_sem=p_send.at[it, n], recv_sem=p_recv.at[it, slot],
                device_id=where, device_id_type=MESH,
            )
            copy.start()
            sent.append(copy)

        if halo_too:
            for n, c in enumerate(across_cols):
                send_product(n, jnp.where(low, 6 + col, col - 2), at_tile(across, c))
        for o in range(1, 4):
            send_product(1 + o, own, (ty, tz, core, lax.rem(col + o, 4)))

        def summed(buf, n):
            acc = buf[it, 0]
            for i in range(1, n):
                acc = acc + buf[it, i]
            return acc

        @pl.when(core == 1)
        def _():
            ra[it, line] = pay[it]
            for o in range(1, 8):
                other = lax.rem(line + o, 8)
                pltpu.make_async_remote_copy(
                    src_ref=pay.at[it], dst_ref=ra.at[it, other], send_sem=a_send.at[it, 0],
                    recv_sem=a_recv.at[it, other], device_id=(ty, tz, 1, col), device_id_type=MESH,
                ).wait_recv()
            rb[it, ty] = summed(ra, 8)

            def along(buf, me, n, send, recv, place):
                copies = []
                for o in sorted(range(1, n), key=lambda o: -min(o, n - o)):
                    copy = pltpu.make_async_remote_copy(
                        src_ref=buf.at[it, me], dst_ref=buf.at[it, me], send_sem=send.at[it, o], recv_sem=recv.at[it, me],
                        device_id=place(lax.rem(me + o, n)), device_id_type=MESH,
                    )
                    copy.start()
                    copies.append(copy)
                for o in range(1, n):
                    other = lax.rem(me + o, n)
                    pltpu.make_async_remote_copy(
                        src_ref=buf.at[it, other], dst_ref=buf.at[it, other], send_sem=send.at[it, o],
                        recv_sem=recv.at[it, other], device_id=place(other), device_id_type=MESH,
                    ).wait_recv()
                return copies

            done = along(rb, ty, ny, b_send, b_recv, lambda i: (i, tz, 1, col))
            rc[it, tz] = summed(rb, ny)
            done += along(rc, tz, nz, c_send, c_recv, lambda i: (ty, i, 1, col))
            tot[it] = summed(rc, nz)
            down = pltpu.make_async_remote_copy(
                src_ref=tot.at[it], dst_ref=tot.at[it], send_sem=t_send.at[it], recv_sem=t_recv.at[it],
                device_id=(ty, tz, 0, col), device_id_type=MESH,
            )
            down.start()
            for copy in done:
                copy.wait_send()
            down.wait_send()

        @pl.when(core == 0)
        def _():
            pltpu.make_async_remote_copy(
                src_ref=tot.at[it], dst_ref=tot.at[it], send_sem=t_send.at[it], recv_sem=t_recv.at[it],
                device_id=(ty, tz, 1, col), device_id_type=MESH,
            ).wait_recv()

        def arrived(slot):
            pltpu.make_async_remote_copy(
                src_ref=pg.at[it, slot], dst_ref=pg.at[it, slot], send_sem=p_send.at[it, 0], recv_sem=p_recv.at[it, slot],
                device_id=(ty, tz, core, lax.rem(col + 1, 4)), device_id_type=MESH,
            ).wait_recv()

        for o in range(1, 4):
            arrived(2 + lax.rem(col + o, 4))
        if halo_too:
            for n in range(2):
                arrived(jnp.where(low, n, 6 + n))
        for copy in sent:
            copy.wait_send()
        for x in range(4):
            @pl.when(jnp.logical_or(core == 0, col != x))
            def _():
                to_line(x).wait_send()

        return jnp.concatenate([tot[it, :, g * 32 : (g + 1) * 32] for g in range(4)], axis=0)

    def updated(it, source, slot, c_hi, c_lo):
        out = []
        for d in range(3):
            x = source[slot, d * 16 : (d + 1) * 16, :]
            hi, lo = split(x)
            kept = mm(c_hi, hi) + mm(c_lo, hi) + mm(c_hi, lo)
            out.append(x - STEP * (pg[it, slot, d * 16 : (d + 1) * 16, :] - kept))
        return out

    here, product = finish_product(gathered, xg)
    z = exchange(0, here, product, True)
    c_hi, c_lo = split(solve(z))
    for i in range(6):
        slot = jnp.where(low, 0, 2) + i
        for d, part in enumerate(updated(0, xg, slot, c_hi, c_lo)):
            x1[slot, d * 16 : (d + 1) * 16, :] = part

    for q in range(5):
        near_vectors(x1, q)
    here, product = finish_product(near_sum(0, 5), x1)
    z = exchange(1, here, product, False)
    coef = solve(z)
    c_hi, c_lo = split(coef)
    for r in range(4):
        for d, part in enumerate(updated(1, x1, 2 + r, c_hi, c_lo)):
            next_ref[d * 16 : (d + 1) * 16, r * 128 : (r + 1) * 128] = part

    corr_ref[...] = z[0:16, 0:16] * scale
    ray_ref[...] = z[0:16, 16:32] * scale
    row = iota((16, 32), 0)
    squares = jnp.sum(jnp.where(iota((16, 32), 1) == row + 16, z[16:32, :], 0.0), axis=1, keepdims=True)
    norms = squares - jnp.sum(z[16:32, 0:16] * coef, axis=1, keepdims=True)
    square = (16, 16)
    norm_ref[...] = jnp.sum(jnp.where(iota(square, 0) == iota(square, 1), norms * scale, 0.0), axis=0, keepdims=True)
    halo.wait_send()


def per_device(ny, nz, positions, trial_block, pair_tiles, pair_count):
    scale = 1.0 / (3.0 * ny * nz * 2 * 512)
    vmem = pl.BlockSpec(memory_space=pltpu.VMEM)
    dma = pltpu.SemaphoreType.DMA
    n = max(ny, nz, 8)
    out = pl.pallas_call(
        functools.partial(kernel, ny, nz, scale),
        out_shape=(
            jax.ShapeDtypeStruct((48, 512), F32),
            jax.ShapeDtypeStruct((16, 16), F32),
            jax.ShapeDtypeStruct((16, 16), F32),
            jax.ShapeDtypeStruct((1, 16), F32),
        ),
        in_specs=[vmem, vmem, vmem, pl.BlockSpec(memory_space=pltpu.SMEM)],
        out_specs=(vmem, vmem, vmem, vmem),
        scratch_shapes=[
            pltpu.VMEM((8, 56, 128), F32),
            pltpu.VMEM((8, 48, 128), F32),
            pltpu.VMEM((2, 8, 48, 128), F32),
            pltpu.VMEM((640, 768), BF16),
            pltpu.VMEM((640, 768), BF16),
            pltpu.VMEM((96, 640), BF16),
            pltpu.VMEM((6, 8, 128), F32),
            pltpu.VMEM((2, 8, 128), F32),
            pltpu.VMEM((2, 8, 8, 128), F32),
            pltpu.VMEM((2, ny, 8, 128), F32),
            pltpu.VMEM((2, nz, 8, 128), F32),
            pltpu.VMEM((2, 8, 128), F32),
            dma, dma,
            dma((2, 8)), dma((2, 8)),
            dma((2, 4)), dma((2, 8)),
            dma((2, n)), dma((2, n)),
            dma((2, n)), dma((2, n)),
            dma((2,)), dma((2,)),
        ],
        compiler_params=pltpu.CompilerParams(collective_id=0, has_side_effects=True),
        name="block_step",
    )(trial_block.reshape(48, 512), positions, pair_tiles.reshape(2, 4, 8), pair_count)
    block, rayleigh, correlation, norms = out
    return block.reshape(3, 16, 512), rayleigh, correlation, norms.reshape(16)


def build(finer):
    return jax.shard_map(
        functools.partial(per_device, finer.shape["ty"], finer.shape["tz"]),
        mesh=finer,
        in_specs=(P(None, TILE), P(None, None, TILE), P(None, TILE, None, None), P(TILE, None)),
        out_specs=(P(None, None, TILE), P(), P(), P()),
        check_vma=False,
    )


def solution(mesh):
    return build(Mesh(mesh.devices.reshape(8, 8, 2, mesh.shape["col"]), (*TILE, "col")))
```

```python
import functools

import jax
import jax.numpy as jnp
from jax import lax
from jax.experimental import pallas as pl
from jax.experimental.pallas import tpu as pltpu
from jax.sharding import Mesh
from jax.sharding import PartitionSpec as P

TILE = ("ty", "tz", "core")
MESH = pl.DeviceIdType.MESH
F32 = jnp.float32
BF16 = jnp.bfloat16
HIGHEST = lax.Precision.HIGHEST

STEP = 0.2
MATS = ((0, 0), (0, 1), (0, 2), (1, 1), (1, 2), (2, 2))
MAT_OF = {(0, 0): 0, (0, 1): 1, (1, 0): 1, (0, 2): 2, (2, 0): 2, (1, 1): 3, (1, 2): 4, (2, 1): 4, (2, 2): 5}


def iota(shape, axis):
    return lax.broadcasted_iota(jnp.int32, shape, axis)


def split(x):
    hi = x.astype(BF16)
    return hi, (x - hi.astype(F32)).astype(BF16)


def mm(a, b):
    return lax.dot_general(a, b, (((1,), (0,)), ((), ())), preferred_element_type=F32)


def mm_exact(a, b, transposed=False):
    dims = (((1,), (1 if transposed else 0,)), ((), ()))
    return lax.dot_general(a, b, dims, precision=HIGHEST, preferred_element_type=F32)


def solve(corr, gram):
    m = jnp.concatenate([corr, gram], axis=0)
    lane = iota((32, 16), 1)
    for j in range(16):
        col = m[:, j : j + 1]
        inv = 1.0 / m[j : j + 1, j : j + 1]
        row = m[j : j + 1, :] * inv
        m = jnp.where(lane == j, col * inv, m - col * row)
    return m[16:32, :]


def finish(scale, xpq_ref, z_ref, next_ref, ray_ref, corr_ref, norm_ref):
    xx, xp, pp, pq = (z_ref[:, 16 * i : 16 * i + 16] for i in range(4))
    qq = z_ref[:, 64:65]
    eye = iota((16, 16), 0) == iota((16, 16), 1)
    one = jnp.where(eye, 1.0, 0.0).astype(F32)
    c0 = solve(xx, xp)
    at = one + STEP * c0
    left = mm_exact(at, jnp.concatenate([xx, xp, pp, pq], axis=1))
    a_xx, a_xp, a_pp, a_pq = (left[:, 16 * i : 16 * i + 16] for i in range(4))
    y1, y2, y3 = a_xx - STEP * xp, a_xp - STEP * pp, a_pp - STEP * pq
    right = mm_exact(jnp.concatenate([y1, y2], axis=0), at, transposed=True)
    corr = right[0:16] - STEP * y2
    gram = right[16:32] - STEP * y3
    c1 = solve(corr, gram)

    both = c0 + c1
    factor = jnp.concatenate([STEP * both + STEP * STEP * mm_exact(c1, c0), -STEP * STEP * both], axis=1)
    f_hi, f_lo = split(factor)
    for r in range(4):
        for d in range(3):
            rows, lanes = slice(d * 16, (d + 1) * 16), slice(r * 128, (r + 1) * 128)
            x, p, q = (xpq_ref[i, r, rows, :] for i in range(3))
            hi, lo = split(jnp.concatenate([x, p], axis=0))
            moved = mm(f_hi, hi) + mm(f_lo, hi) + mm(f_hi, lo)
            next_ref[rows, lanes] = (x - 2.0 * STEP * p) + (moved + STEP * STEP * q)

    corr_ref[...] = corr * scale
    ray_ref[...] = gram * scale
    squares = jnp.sum(a_pp * at - 2.0 * STEP * jnp.where(eye, a_pq, 0.0), axis=1, keepdims=True) + STEP * STEP * qq
    norms = (squares - jnp.sum(gram * c1, axis=1, keepdims=True)) * scale
    norm_ref[...] = jnp.sum(jnp.where(eye, norms, 0.0), axis=0, keepdims=True)


def kernel(
    ny, nz,
    x_hbm, pos_hbm, pairs_hbm, count_hbm,
    xpq_ref, z_ref,
    pos_ref, pairs_ref, count_ref, in_sem,
    xg, pg, qg, shi, slo, lw, dacc, pay, ra, rb, rc,
    halo_send, halo_recv, p_send, p_recv, q_send, q_recv, a_send, a_recv, b_send, b_recv, c_send, c_recv,
):
    ty, tz, core, col = (lax.axis_index(n) for n in ("ty", "tz", "core", "col"))
    tiles = ny * nz * 2
    t = (ty * nz + tz) * 2 + core
    low = col < 2

    def at_tile(index, c):
        return (lax.div(index, 2 * nz), lax.rem(lax.div(index, 2), nz), lax.rem(index, 2), c)

    after, before = lax.rem(t + 1, tiles), lax.rem(t + tiles - 1, tiles)
    across = jnp.where(low, before, after)
    across_cols = (jnp.where(low, 2, 0), jnp.where(low, 3, 1))

    fetches = [
        pltpu.make_async_copy(count_hbm, count_ref, in_sem.at[0]),
        pltpu.make_async_copy(pairs_hbm, pairs_ref, in_sem.at[1]),
        pltpu.make_async_copy(pos_hbm, pos_ref, in_sem.at[2]),
    ]
    for r in range(4):
        lanes = slice(r * 128, (r + 1) * 128)
        fetches.append(pltpu.make_async_copy(x_hbm.at[:, lanes], xg.at[2 + r, 0:48, :], in_sem.at[3 + r]))
    for fetch in fetches:
        fetch.start()

    barrier = pltpu.get_barrier_semaphore()

    def greet(where):
        pl.semaphore_signal(barrier, inc=1, device_id=where, device_id_type=MESH)

    @pl.when(core == 1)
    def _():
        for o in range(1, ny):
            greet((lax.rem(ty + o, ny), tz, core, col))
        for o in range(1, nz):
            greet((ty, lax.rem(tz + o, nz), core, col))

    @pl.when(core == 0)
    def _():
        for o in range(1, nz):
            greet((ty, lax.rem(tz + o, nz), 1, col))

    for c in across_cols:
        greet(at_tile(across, c))
    greet(at_tile(after, col))
    greet(at_tile(before, col))
    for o in range(1, 4):
        greet((ty, tz, core, lax.rem(col + o, 4)))
        greet((ty, tz, 1 - core, lax.rem(col + o, 4)))
    greet((ty, tz, 1 - core, col))

    for fetch in fetches:
        fetch.wait()
    lane = iota((1, 128), 1)
    rows, cols = pairs_ref[0], pairs_ref[1]
    slot_col = iota((4, 8), 0)
    counts = jnp.zeros((4, 8), jnp.int32)
    for c in range(4):
        counts = jnp.where(slot_col == c, count_ref[:, c : c + 1], counts)
    live = jnp.where(iota((4, 8), 1) < counts, 1.0, 0.0).astype(F32)
    reach = cols - t * 4 - rows
    for r in range(4):
        xg[2 + r, 48:56, :] = jnp.zeros((8, 128), F32)
        xg[2 + r, 48:51, :] = pos_ref[:, r * 128 : (r + 1) * 128]
        listed = jnp.zeros((1, 128), F32)
        for k in range(3):
            here = jnp.where((rows == r) & (reach == k), live, 0.0)
            total = jnp.sum(jnp.sum(here, axis=1, keepdims=True), axis=0, keepdims=True)
            listed = jnp.where(lane == k, total, listed)
        xg[2 + r, 51:52, :] = listed

    dacc[...] = jnp.zeros_like(dacc)
    own = 2 + col

    def spring_block(q, slot):
        mine = [xg[own, 48 + d : 49 + d, :] for d in range(3)]
        listed = xg[jnp.minimum(slot, own), 51:52, :]
        times = jnp.sum(jnp.where(lane == jnp.abs(slot - own), listed, 0.0), axis=1, keepdims=True)
        times = times * (1.0 / 64.0)
        near = jnp.transpose(xg[slot, 48:56, :])
        sums = [dacc[m] for m in range(6)]
        for ch in range(4):
            part = near[ch * 32 : (ch + 1) * 32]
            off = [part[:, d : d + 1] - mine[d] for d in range(3)]
            dist = off[0] * off[0] + off[1] * off[1] + off[2] * off[2]
            fall = 1.0 - dist * (1.0 / 225.0)
            weight = jnp.where(dist < 225.0, fall * fall, 0.0) * times / jnp.maximum(dist, 1.0)
            by = [weight * o for o in off]
            at = pl.ds(pl.multiple_of(q * 128 + ch * 32, 32), 32)
            for m, (c, d) in enumerate(MATS):
                s = by[c] * off[d]
                hi, lo = split(s)
                shi[at, m * 128 : (m + 1) * 128] = hi
                slo[at, m * 128 : (m + 1) * 128] = lo
                sums[m] = sums[m] + ((s[0:8] + s[8:16]) + (s[16:24] + s[24:32]))
        for m in range(6):
            dacc[m] = sums[m]

    first = jnp.where(low, 2, 3)
    late = (
        jnp.where(col == 0, 0, jnp.where(col == 1, 1, jnp.where(col == 2, 2, 6))),
        jnp.where(col == 0, 1, jnp.where(col == 1, 5, jnp.where(col == 2, 6, 7))),
    )
    slots = (first, first + 1, first + 2) + late

    pl.semaphore_wait(barrier, 11 + core * (ny + 2 * nz - 3))
    from_slot, to_slot = jnp.where(low, 4, 2), jnp.where(low, 0, 6)
    halo = pltpu.make_async_remote_copy(
        src_ref=xg.at[pl.ds(from_slot, 2)],
        dst_ref=xg.at[pl.ds(to_slot, 2)],
        send_sem=halo_send,
        recv_sem=halo_recv,
        device_id=at_tile(jnp.where(low, after, before), col),
        device_id_type=MESH,
    )
    halo.start()

    def near_vectors(source, q):
        hi, lo = split(source[slots[q], 0:48, :])
        lw[0:48, q * 128 : (q + 1) * 128] = hi
        lw[48:96, q * 128 : (q + 1) * 128] = lo

    def near_sum(start, stop):
        a, b = start * 128, stop * 128
        both = mm(lw[:, a:b], shi[a:b, :])
        return both[0:48] + both[48:96] + mm(lw[0:48, a:b], slo[a:b, :])

    def first_blocks(q, carry):
        spring_block(q, first + q)
        return carry

    lax.fori_loop(0, 3, first_blocks, 0)
    for q in range(3):
        near_vectors(xg, q)
    gathered = near_sum(0, 3)
    halo.wait_recv()

    def late_blocks(q, carry):
        spring_block(3 + q, jnp.where(q == 0, late[0], late[1]))
        return carry

    lax.fori_loop(0, 2, late_blocks, 0)
    for q in range(3, 5):
        near_vectors(xg, q)
    gathered = gathered + near_sum(3, 5)
    diag = [jnp.sum(dacc[m], axis=0, keepdims=True) for m in range(6)]

    def finish_product(gathered, source):
        here = [source[own, d * 16 : (d + 1) * 16, :] for d in range(3)]
        out = []
        for c in range(3):
            acc = None
            for d in range(3):
                m = MAT_OF[(c, d)]
                term = diag[m] * here[d] - gathered[d * 16 : (d + 1) * 16, m * 128 : (m + 1) * 128]
                acc = term if acc is None else acc + term
            out.append(acc)
        return here, out

    def moved(buf, at, send, recv, where):
        return pltpu.make_async_remote_copy(
            src_ref=buf.at[at], dst_ref=buf.at[at], send_sem=send, recv_sem=recv, device_id=where, device_id_type=MESH
        )

    here, first_product = finish_product(gathered, xg)
    for d in range(3):
        pg[own, d * 16 : (d + 1) * 16, :] = first_product[d]
    sent = []
    for n, c in enumerate(across_cols):
        sent.append(
            pltpu.make_async_remote_copy(
                src_ref=pg.at[own], dst_ref=pg.at[jnp.where(low, 6 + col, col - 2)], send_sem=p_send.at[n],
                recv_sem=p_recv.at[jnp.where(low, 6 + col, col - 2)], device_id=at_tile(across, c), device_id_type=MESH,
            )
        )
    for o in range(1, 4):
        sent.append(moved(pg, own, p_send.at[1 + o], p_recv.at[own], (ty, tz, core, lax.rem(col + o, 4))))
    for copy in sent:
        copy.start()

    def arrived(buf, slot, recv):
        moved(buf, slot, p_send.at[0], recv, (ty, tz, core, lax.rem(col + 1, 4))).wait_recv()

    for o in range(1, 4):
        other = 2 + lax.rem(col + o, 4)
        arrived(pg, other, p_recv.at[other])
    for n in range(2):
        other = jnp.where(low, n, 6 + n)
        arrived(pg, other, p_recv.at[other])

    for q in range(5):
        near_vectors(pg, q)
    _, second_product = finish_product(near_sum(0, 5), pg)

    for d in range(3):
        qg[col, d * 16 : (d + 1) * 16, :] = second_product[d]
    x, p, q = (jnp.concatenate(parts, axis=1) for parts in (here, first_product, second_product))
    z = mm_exact(jnp.concatenate([x, p], axis=0), jnp.concatenate([x, p, q], axis=0), transposed=True)
    pay[:, 0:32] = z[0:16, 0:32]
    pay[:, 32:64] = z[16:32, 16:48]
    pay[:, 64:128] = jnp.broadcast_to(jnp.sum(q * q, axis=1, keepdims=True), (16, 64))

    line = col * 2 + core

    def to_line(x):
        return pltpu.make_async_remote_copy(
            src_ref=pay, dst_ref=ra.at[line], send_sem=a_send.at[x], recv_sem=a_recv.at[line],
            device_id=(ty, tz, 1, x), device_id_type=MESH,
        )

    for x in range(4):
        @pl.when(jnp.logical_or(core == 0, col != x))
        def _():
            to_line(x).start()

    for o in range(1, 4):
        copy = moved(qg, col, q_send.at[o - 1], q_recv.at[col], (ty, tz, core, lax.rem(col + o, 4)))
        copy.start()
        sent.append(copy)

    def summed(buf, n):
        parts = [buf[i] for i in range(n)]
        while len(parts) > 1:
            parts = [a + b for a, b in zip(parts[0::2], parts[1::2])] + parts[len(parts) & ~1 :]
        return parts[0]

    def far_first(n):
        return sorted(range(1, n), key=lambda o: -min(o, n - o))

    @pl.when(core == 1)
    def _():
        ra[line] = pay[...]
        for o in range(1, 8):
            other = lax.rem(line + o, 8)
            moved(ra, other, a_send.at[0], a_recv.at[other], (ty, tz, 0, col)).wait_recv()
        rb[ty] = summed(ra, 8)
        done = []
        for o in far_first(ny):
            done.append(moved(rb, ty, b_send.at[o], b_recv.at[ty], (lax.rem(ty + o, ny), tz, 1, col)))
            done[-1].start()
        for o in range(1, ny):
            other = lax.rem(ty + o, ny)
            moved(rb, other, b_send.at[o], b_recv.at[other], (other, tz, 1, col)).wait_recv()
        rc[tz] = summed(rb, ny)
        for o in far_first(nz) + [0]:
            place = lax.rem(tz + o, nz)
            done.append(moved(rc, tz, c_send.at[0, o], c_recv.at[tz], (ty, place, 0, col)))
            done[-1].start()
            if o:
                done.append(moved(rc, tz, c_send.at[1, o], c_recv.at[tz], (ty, place, 1, col)))
                done[-1].start()
        for o in range(1, nz):
            other = lax.rem(tz + o, nz)
            moved(rc, other, c_send.at[0, 0], c_recv.at[other], (ty, tz, 0, col)).wait_recv()
        for copy in done:
            copy.wait_send()

    @pl.when(core == 0)
    def _():
        for other in range(nz):
            moved(rc, other, c_send.at[0, 0], c_recv.at[other], (ty, tz, 1, col)).wait_recv()

    z_ref[...] = summed(rc, nz)
    for o in range(1, 4):
        other = lax.rem(col + o, 4)
        arrived(qg, other, q_recv.at[other])
    for r in range(4):
        xpq_ref[0, r] = xg[2 + r, 0:48, :]
        xpq_ref[1, r] = pg[2 + r]
        xpq_ref[2, r] = qg[r]
    for copy in sent:
        copy.wait_send()
    for x in range(4):
        @pl.when(jnp.logical_or(core == 0, col != x))
        def _():
            to_line(x).wait_send()
    halo.wait_send()


def per_device(ny, nz, positions, trial_block, pair_tiles, pair_count):
    scale = 1.0 / (3.0 * ny * nz * 2 * 512)
    vmem = pl.BlockSpec(memory_space=pltpu.VMEM)
    dma = pltpu.SemaphoreType.DMA
    hbm = pl.BlockSpec(memory_space=pltpu.HBM)
    products, gram = pl.pallas_call(
        functools.partial(kernel, ny, nz),
        out_shape=(jax.ShapeDtypeStruct((3, 4, 48, 128), F32), jax.ShapeDtypeStruct((16, 128), F32)),
        in_specs=[hbm] * 4,
        out_specs=(vmem, vmem),
        scratch_shapes=[
            pltpu.VMEM((3, 512), F32),
            pltpu.VMEM((2, 4, 8), jnp.int32),
            pltpu.VMEM((1, 4), jnp.int32),
            dma((7,)),
            pltpu.VMEM((8, 56, 128), F32),
            pltpu.VMEM((8, 48, 128), F32),
            pltpu.VMEM((4, 48, 128), F32),
            pltpu.VMEM((640, 768), BF16),
            pltpu.VMEM((640, 768), BF16),
            pltpu.VMEM((96, 640), BF16),
            pltpu.VMEM((6, 8, 128), F32),
            pltpu.VMEM((16, 128), F32),
            pltpu.VMEM((8, 16, 128), F32),
            pltpu.VMEM((ny, 16, 128), F32),
            pltpu.VMEM((nz, 16, 128), F32),
            dma, dma,
            dma((5,)), dma((8,)),
            dma((3,)), dma((4,)),
            dma((4,)), dma((8,)),
            dma((ny,)), dma((ny,)),
            dma((2, nz)), dma((nz,)),
        ],
        compiler_params=pltpu.CompilerParams(collective_id=0, has_side_effects=True, vmem_limit_bytes=16 << 20),
        name="gram_blocks",
    )(trial_block.reshape(48, 512), positions, pair_tiles.reshape(2, 4, 8), pair_count)
    block, rayleigh, correlation, norms = pl.pallas_call(
        functools.partial(finish, scale),
        out_shape=(
            jax.ShapeDtypeStruct((48, 512), F32),
            jax.ShapeDtypeStruct((16, 16), F32),
            jax.ShapeDtypeStruct((16, 16), F32),
            jax.ShapeDtypeStruct((1, 16), F32),
        ),
        in_specs=[vmem] * 2,
        out_specs=(vmem,) * 4,
        compiler_params=pltpu.CompilerParams(vmem_limit_bytes=16 << 20),
        name="finish",
    )(products, gram)
    return block.reshape(3, 16, 512), rayleigh, correlation, norms.reshape(16)


def build(finer):
    return jax.shard_map(
        functools.partial(per_device, finer.shape["ty"], finer.shape["tz"]),
        mesh=finer,
        in_specs=(P(None, TILE), P(None, None, TILE), P(None, TILE, None, None), P(TILE, None)),
        out_specs=(P(None, None, TILE), P(), P(), P()),
        check_vma=False,
    )


def solution(mesh):
    return build(Mesh(mesh.devices.reshape(8, 8, 2, mesh.shape["col"]), (*TILE, "col")))
```

```python
import functools

import jax
import jax.numpy as jnp
from jax import lax
from jax.experimental import pallas as pl
from jax.experimental.pallas import tpu as pltpu
from jax.sharding import Mesh
from jax.sharding import PartitionSpec as P

TILE = ("ty", "tz", "core")
MESH = pl.DeviceIdType.MESH
F32 = jnp.float32
BF16 = jnp.bfloat16
HIGHEST = lax.Precision.HIGHEST

STEP = 0.2
MATS = ((0, 0), (0, 1), (0, 2), (1, 1), (1, 2), (2, 2))
MAT_OF = {(0, 0): 0, (0, 1): 1, (1, 0): 1, (0, 2): 2, (2, 0): 2, (1, 1): 3, (1, 2): 4, (2, 1): 4, (2, 2): 5}


def iota(shape, axis):
    return lax.broadcasted_iota(jnp.int32, shape, axis)


def split(x):
    hi = x.astype(BF16)
    return hi, (x - hi.astype(F32)).astype(BF16)


def mm(a, b):
    return lax.dot_general(a, b, (((1,), (0,)), ((), ())), preferred_element_type=F32)


def mm_exact(a, b, transposed=False):
    dims = (((1,), (1 if transposed else 0,)), ((), ()))
    return lax.dot_general(a, b, dims, precision=HIGHEST, preferred_element_type=F32)


def solve(corr, gram):
    m = jnp.concatenate([corr, gram], axis=0)
    shape = (32, 16)
    lane = iota(shape, 1)
    wide = [jnp.broadcast_to(m[:, j : j + 1], shape) for j in range(16)]
    for j in range(16):
        col = wide[j] / jnp.broadcast_to(wide[j][j : j + 1, :], shape)
        m = jnp.where(lane == j, col, m - col * jnp.broadcast_to(m[j : j + 1, :], shape))
        for n in range(j + 1, 16):
            wide[n] = wide[n] - col * jnp.broadcast_to(wide[n][j : j + 1, :], shape)
    return m[16:32, :]


def finish(scale, x_hbm, pq_hbm, z_hbm, next_ref, ray_ref, corr_ref, norm_ref, x_ref, pq_ref, z_ref, in_sem):
    gram_in = pltpu.make_async_copy(z_hbm, z_ref, in_sem.at[0])
    x_in = pltpu.make_async_copy(x_hbm, x_ref, in_sem.at[1])
    pq_in = pltpu.make_async_copy(pq_hbm, pq_ref, in_sem.at[2])
    for copy in (gram_in, x_in, pq_in):
        copy.start()
    gram_in.wait()
    xx, xp, pp, pq = (z_ref[:, 16 * i : 16 * i + 16] for i in range(4))
    qq = z_ref[:, 64:65]
    eye = iota((16, 16), 0) == iota((16, 16), 1)
    one = jnp.where(eye, 1.0, 0.0).astype(F32)
    c0 = solve(xx, xp)
    at = one + STEP * c0
    left = mm_exact(at, jnp.concatenate([xx, xp, pp, pq], axis=1))
    a_xx, a_xp, a_pp, a_pq = (left[:, 16 * i : 16 * i + 16] for i in range(4))
    y1, y2, y3 = a_xx - STEP * xp, a_xp - STEP * pp, a_pp - STEP * pq
    right = mm_exact(jnp.concatenate([y1, y2], axis=0), at, transposed=True)
    corr = right[0:16] - STEP * y2
    gram = right[16:32] - STEP * y3
    c1 = solve(corr, gram)

    both = c0 + c1
    factor = jnp.concatenate([STEP * both + STEP * STEP * mm_exact(c1, c0), -STEP * STEP * both], axis=1)
    f_hi, f_lo = split(factor)
    x_in.wait()
    pq_in.wait()
    for r in range(4):
        for d in range(3):
            rows, lanes = slice(d * 16, (d + 1) * 16), slice(r * 128, (r + 1) * 128)
            x, p, q = x_ref[rows, lanes], pq_ref[0, r, rows, :], pq_ref[1, r, rows, :]
            hi, lo = split(jnp.concatenate([x, p], axis=0))
            moved = mm(f_hi, hi) + mm(f_lo, hi) + mm(f_hi, lo)
            next_ref[rows, lanes] = (x - 2.0 * STEP * p) + (moved + STEP * STEP * q)

    corr_ref[...] = corr * scale
    ray_ref[...] = gram * scale
    squares = jnp.sum(a_pp * at - 2.0 * STEP * jnp.where(eye, a_pq, 0.0), axis=1, keepdims=True) + STEP * STEP * qq
    norms = (squares - jnp.sum(gram * c1, axis=1, keepdims=True)) * scale
    norm_ref[...] = jnp.sum(jnp.where(eye, norms, 0.0), axis=0, keepdims=True)


def kernel(
    ny, nz,
    x_hbm, pos_hbm, pairs_hbm, count_hbm,
    pq_hbm, z_hbm,
    pos_ref, pairs_ref, count_ref, in_sem, z_ref, out_sem,
    xg, pg, qg, shi, slo, lw, dacc, pay, ra, rb, rc,
    halo_send, halo_recv, p_send, p_recv, q_send, q_recv, a_send, a_recv, b_send, b_recv, c_send, c_recv,
):
    ty, tz, core, col = (lax.axis_index(n) for n in ("ty", "tz", "core", "col"))
    tiles = ny * nz * 2
    t = (ty * nz + tz) * 2 + core
    low = col < 2

    def at_tile(index, c):
        return (lax.div(index, 2 * nz), lax.rem(lax.div(index, 2), nz), lax.rem(index, 2), c)

    after, before = lax.rem(t + 1, tiles), lax.rem(t + tiles - 1, tiles)
    across = jnp.where(low, before, after)
    across_cols = (jnp.where(low, 2, 0), jnp.where(low, 3, 1))

    fetches = [
        pltpu.make_async_copy(count_hbm, count_ref, in_sem.at[0]),
        pltpu.make_async_copy(pairs_hbm, pairs_ref, in_sem.at[1]),
        pltpu.make_async_copy(pos_hbm, pos_ref, in_sem.at[2]),
    ]
    for r in range(4):
        lanes = slice(r * 128, (r + 1) * 128)
        fetches.append(pltpu.make_async_copy(x_hbm.at[:, lanes], xg.at[2 + r, 0:48, :], in_sem.at[3 + r]))
    for fetch in fetches:
        fetch.start()

    barrier = pltpu.get_barrier_semaphore()

    def greet(where):
        pl.semaphore_signal(barrier, inc=1, device_id=where, device_id_type=MESH)

    @pl.when(core == 1)
    def _():
        for o in range(1, ny):
            greet((lax.rem(ty + o, ny), tz, core, col))
        for o in range(1, nz):
            greet((ty, lax.rem(tz + o, nz), core, col))

    @pl.when(core == 0)
    def _():
        for o in range(1, nz):
            greet((ty, lax.rem(tz + o, nz), 1, col))

    for c in across_cols:
        greet(at_tile(across, c))
    greet(at_tile(after, col))
    greet(at_tile(before, col))
    for o in range(1, 4):
        greet((ty, tz, core, lax.rem(col + o, 4)))
        greet((ty, tz, 1 - core, lax.rem(col + o, 4)))
    greet((ty, tz, 1 - core, col))

    for fetch in fetches:
        fetch.wait()
    lane = iota((1, 128), 1)
    rows, cols = pairs_ref[0], pairs_ref[1]
    slot_col = iota((4, 8), 0)
    counts = jnp.zeros((4, 8), jnp.int32)
    for c in range(4):
        counts = jnp.where(slot_col == c, count_ref[:, c : c + 1], counts)
    live = jnp.where(iota((4, 8), 1) < counts, 1.0, 0.0).astype(F32)
    reach = cols - t * 4 - rows
    for r in range(4):
        xg[2 + r, 48:56, :] = jnp.zeros((8, 128), F32)
        xg[2 + r, 48:51, :] = pos_ref[:, r * 128 : (r + 1) * 128]
        listed = jnp.zeros((1, 128), F32)
        for k in range(3):
            here = jnp.where((rows == r) & (reach == k), live, 0.0)
            total = jnp.sum(jnp.sum(here, axis=1, keepdims=True), axis=0, keepdims=True)
            listed = jnp.where(lane == k, total, listed)
        xg[2 + r, 51:52, :] = listed

    dacc[...] = jnp.zeros_like(dacc)
    own = 2 + col

    def spring_block(q, slot):
        mine = [xg[own, 48 + d : 49 + d, :] for d in range(3)]
        listed = xg[jnp.minimum(slot, own), 51:52, :]
        times = jnp.sum(jnp.where(lane == jnp.abs(slot - own), listed, 0.0), axis=1, keepdims=True)
        times = times * (1.0 / 64.0)
        near = jnp.transpose(xg[slot, 48:56, :])
        sums = [dacc[m] for m in range(6)]
        for ch in range(4):
            part = near[ch * 32 : (ch + 1) * 32]
            off = [part[:, d : d + 1] - mine[d] for d in range(3)]
            dist = off[0] * off[0] + off[1] * off[1] + off[2] * off[2]
            fall = 1.0 - dist * (1.0 / 225.0)
            weight = jnp.where(dist < 225.0, fall * fall, 0.0) * times / jnp.maximum(dist, 1.0)
            by = [weight * o for o in off]
            at = pl.ds(pl.multiple_of(q * 128 + ch * 32, 32), 32)
            for m, (c, d) in enumerate(MATS):
                s = by[c] * off[d]
                hi, lo = split(s)
                shi[at, m * 128 : (m + 1) * 128] = hi
                slo[at, m * 128 : (m + 1) * 128] = lo
                sums[m] = sums[m] + ((s[0:8] + s[8:16]) + (s[16:24] + s[24:32]))
        for m in range(6):
            dacc[m] = sums[m]

    first = jnp.where(low, 2, 3)
    late = (
        jnp.where(col == 0, 0, jnp.where(col == 1, 1, jnp.where(col == 2, 2, 6))),
        jnp.where(col == 0, 1, jnp.where(col == 1, 5, jnp.where(col == 2, 6, 7))),
    )
    slots = (first, first + 1, first + 2) + late

    pl.semaphore_wait(barrier, 11 + core * (ny + 2 * nz - 3))
    from_slot, to_slot = jnp.where(low, 4, 2), jnp.where(low, 0, 6)
    halo = pltpu.make_async_remote_copy(
        src_ref=xg.at[pl.ds(from_slot, 2)],
        dst_ref=xg.at[pl.ds(to_slot, 2)],
        send_sem=halo_send,
        recv_sem=halo_recv,
        device_id=at_tile(jnp.where(low, after, before), col),
        device_id_type=MESH,
    )
    halo.start()

    def near_vectors(source, q):
        hi, lo = split(source[slots[q], 0:48, :])
        lw[0:48, q * 128 : (q + 1) * 128] = hi
        lw[48:96, q * 128 : (q + 1) * 128] = lo

    def near_sum(start, stop):
        a, b = start * 128, stop * 128
        both = mm(lw[:, a:b], shi[a:b, :])
        return both[0:48] + both[48:96] + mm(lw[0:48, a:b], slo[a:b, :])

    def first_blocks(q, carry):
        spring_block(q, first + q)
        return carry

    lax.fori_loop(0, 3, first_blocks, 0)
    for q in range(3):
        near_vectors(xg, q)
    gathered = near_sum(0, 3)
    halo.wait_recv()

    def late_blocks(q, carry):
        spring_block(3 + q, jnp.where(q == 0, late[0], late[1]))
        return carry

    lax.fori_loop(0, 2, late_blocks, 0)
    for q in range(3, 5):
        near_vectors(xg, q)
    gathered = gathered + near_sum(3, 5)
    diag = [jnp.sum(dacc[m], axis=0, keepdims=True) for m in range(6)]

    def finish_product(gathered, source):
        here = [source[own, d * 16 : (d + 1) * 16, :] for d in range(3)]
        out = []
        for c in range(3):
            acc = None
            for d in range(3):
                m = MAT_OF[(c, d)]
                term = diag[m] * here[d] - gathered[d * 16 : (d + 1) * 16, m * 128 : (m + 1) * 128]
                acc = term if acc is None else acc + term
            out.append(acc)
        return here, out

    def moved(buf, at, send, recv, where):
        return pltpu.make_async_remote_copy(
            src_ref=buf.at[at], dst_ref=buf.at[at], send_sem=send, recv_sem=recv, device_id=where, device_id_type=MESH
        )

    here, first_product = finish_product(gathered, xg)
    for d in range(3):
        pg[own, d * 16 : (d + 1) * 16, :] = first_product[d]
    sent = []
    for n, c in enumerate(across_cols):
        sent.append(
            pltpu.make_async_remote_copy(
                src_ref=pg.at[own], dst_ref=pg.at[jnp.where(low, 6 + col, col - 2)], send_sem=p_send.at[n],
                recv_sem=p_recv.at[jnp.where(low, 6 + col, col - 2)], device_id=at_tile(across, c), device_id_type=MESH,
            )
        )
    for o in range(1, 4):
        sent.append(moved(pg, own, p_send.at[1 + o], p_recv.at[own], (ty, tz, core, lax.rem(col + o, 4))))
    for copy in sent:
        copy.start()

    def arrived(buf, slot, recv):
        moved(buf, slot, p_send.at[0], recv, (ty, tz, core, lax.rem(col + 1, 4))).wait_recv()

    for o in range(1, 4):
        other = 2 + lax.rem(col + o, 4)
        arrived(pg, other, p_recv.at[other])
    for n in range(2):
        other = jnp.where(low, n, 6 + n)
        arrived(pg, other, p_recv.at[other])

    for q in range(5):
        near_vectors(pg, q)
    _, second_product = finish_product(near_sum(0, 5), pg)

    for d in range(3):
        qg[col, d * 16 : (d + 1) * 16, :] = second_product[d]
    x, p, q = (jnp.concatenate(parts, axis=1) for parts in (here, first_product, second_product))
    z = mm_exact(jnp.concatenate([x, p], axis=0), jnp.concatenate([x, p, q], axis=0), transposed=True)
    pay[:, 0:32] = z[0:16, 0:32]
    pay[:, 32:64] = z[16:32, 16:48]
    pay[:, 64:128] = jnp.broadcast_to(jnp.sum(q * q, axis=1, keepdims=True), (16, 64))

    line = col * 2 + core

    def to_line(x):
        return pltpu.make_async_remote_copy(
            src_ref=pay, dst_ref=ra.at[line], send_sem=a_send.at[x], recv_sem=a_recv.at[line],
            device_id=(ty, tz, 1, x), device_id_type=MESH,
        )

    for x in range(4):
        @pl.when(jnp.logical_or(core == 0, col != x))
        def _():
            to_line(x).start()

    for o in range(1, 4):
        copy = moved(qg, col, q_send.at[o - 1], q_recv.at[col], (ty, tz, core, lax.rem(col + o, 4)))
        copy.start()
        sent.append(copy)

    def summed(buf, n):
        parts = [buf[i] for i in range(n)]
        while len(parts) > 1:
            parts = [a + b for a, b in zip(parts[0::2], parts[1::2])] + parts[len(parts) & ~1 :]
        return parts[0]

    def far_first(n):
        return sorted(range(1, n), key=lambda o: -min(o, n - o))

    products_out = (
        pltpu.make_async_copy(pg.at[2:6], pq_hbm.at[0], out_sem.at[1]),
        pltpu.make_async_copy(qg, pq_hbm.at[1], out_sem.at[2]),
    )

    def put_products():
        for o in range(1, 4):
            other = lax.rem(col + o, 4)
            arrived(qg, other, q_recv.at[other])
        for copy in products_out:
            copy.start()

    @pl.when(core == 1)
    def _():
        ra[line] = pay[...]
        for o in range(1, 8):
            other = lax.rem(line + o, 8)
            moved(ra, other, a_send.at[0], a_recv.at[other], (ty, tz, 0, col)).wait_recv()
        rb[ty] = summed(ra, 8)
        done = []
        for o in far_first(ny):
            done.append(moved(rb, ty, b_send.at[o], b_recv.at[ty], (lax.rem(ty + o, ny), tz, 1, col)))
            done[-1].start()
        put_products()
        for o in range(1, ny):
            other = lax.rem(ty + o, ny)
            moved(rb, other, b_send.at[o], b_recv.at[other], (other, tz, 1, col)).wait_recv()
        rc[tz] = summed(rb, ny)
        for o in far_first(nz) + [0]:
            place = lax.rem(tz + o, nz)
            done.append(moved(rc, tz, c_send.at[0, o], c_recv.at[tz], (ty, place, 0, col)))
            done[-1].start()
            if o:
                done.append(moved(rc, tz, c_send.at[1, o], c_recv.at[tz], (ty, place, 1, col)))
                done[-1].start()
        for o in range(1, nz):
            other = lax.rem(tz + o, nz)
            moved(rc, other, c_send.at[0, 0], c_recv.at[other], (ty, tz, 0, col)).wait_recv()
        for copy in done:
            copy.wait_send()

    @pl.when(core == 0)
    def _():
        put_products()
        for other in range(nz):
            moved(rc, other, c_send.at[0, 0], c_recv.at[other], (ty, tz, 1, col)).wait_recv()

    z_ref[...] = summed(rc, nz)
    gram_out = pltpu.make_async_copy(z_ref, z_hbm, out_sem.at[0])
    gram_out.start()
    for copy in sent:
        copy.wait_send()
    for x in range(4):
        @pl.when(jnp.logical_or(core == 0, col != x))
        def _():
            to_line(x).wait_send()
    halo.wait_send()
    gram_out.wait()
    for copy in products_out:
        copy.wait()


def per_device(ny, nz, positions, trial_block, pair_tiles, pair_count):
    scale = 1.0 / (3.0 * ny * nz * 2 * 512)
    vmem = pl.BlockSpec(memory_space=pltpu.VMEM)
    dma = pltpu.SemaphoreType.DMA
    hbm = pl.BlockSpec(memory_space=pltpu.HBM)
    block = trial_block.reshape(48, 512)
    products, gram = pl.pallas_call(
        functools.partial(kernel, ny, nz),
        out_shape=(jax.ShapeDtypeStruct((2, 4, 48, 128), F32), jax.ShapeDtypeStruct((16, 128), F32)),
        in_specs=[hbm] * 4,
        out_specs=(hbm, hbm),
        scratch_shapes=[
            pltpu.VMEM((3, 512), F32),
            pltpu.VMEM((2, 4, 8), jnp.int32),
            pltpu.VMEM((1, 4), jnp.int32),
            dma((7,)),
            pltpu.VMEM((16, 128), F32),
            dma((3,)),
            pltpu.VMEM((8, 56, 128), F32),
            pltpu.VMEM((8, 48, 128), F32),
            pltpu.VMEM((4, 48, 128), F32),
            pltpu.VMEM((640, 768), BF16),
            pltpu.VMEM((640, 768), BF16),
            pltpu.VMEM((96, 640), BF16),
            pltpu.VMEM((6, 8, 128), F32),
            pltpu.VMEM((16, 128), F32),
            pltpu.VMEM((8, 16, 128), F32),
            pltpu.VMEM((ny, 16, 128), F32),
            pltpu.VMEM((nz, 16, 128), F32),
            dma, dma,
            dma((5,)), dma((8,)),
            dma((3,)), dma((4,)),
            dma((4,)), dma((8,)),
            dma((ny,)), dma((ny,)),
            dma((2, nz)), dma((nz,)),
        ],
        compiler_params=pltpu.CompilerParams(collective_id=0, has_side_effects=True, vmem_limit_bytes=60 * 1024 * 1024),
        name="gram_blocks",
    )(block, positions, pair_tiles.reshape(2, 4, 8), pair_count)
    block, rayleigh, correlation, norms = pl.pallas_call(
        functools.partial(finish, scale),
        out_shape=(
            jax.ShapeDtypeStruct((48, 512), F32),
            jax.ShapeDtypeStruct((16, 16), F32),
            jax.ShapeDtypeStruct((16, 16), F32),
            jax.ShapeDtypeStruct((1, 16), F32),
        ),
        in_specs=[hbm] * 3,
        out_specs=(vmem,) * 4,
        scratch_shapes=[pltpu.VMEM((48, 512), F32), pltpu.VMEM((2, 4, 48, 128), F32), pltpu.VMEM((16, 128), F32), dma((3,))],
        compiler_params=pltpu.CompilerParams(vmem_limit_bytes=60 * 1024 * 1024),
        name="finish",
    )(block, products, gram)
    return block.reshape(3, 16, 512), rayleigh, correlation, norms.reshape(16)


def build(finer):
    return jax.shard_map(
        functools.partial(per_device, finer.shape["ty"], finer.shape["tz"]),
        mesh=finer,
        in_specs=(P(None, TILE), P(None, None, TILE), P(None, TILE, None, None), P(TILE, None)),
        out_specs=(P(None, None, TILE), P(), P(), P()),
        check_vma=False,
    )


def solution(mesh):
    return build(Mesh(mesh.devices.reshape(8, 8, 2, mesh.shape["col"]), (*TILE, "col")))
```

```python
import functools

import jax
import jax.numpy as jnp
from jax import lax
from jax.experimental import pallas as pl
from jax.experimental.pallas import tpu as pltpu
from jax.sharding import Mesh
from jax.sharding import PartitionSpec as P

TILE = ("ty", "tz", "core")
MESH = pl.DeviceIdType.MESH
F32 = jnp.float32
BF16 = jnp.bfloat16
HIGHEST = lax.Precision.HIGHEST

STEP = 0.2
MATS = ((0, 0), (0, 1), (0, 2), (1, 1), (1, 2), (2, 2))
MAT_OF = {(0, 0): 0, (0, 1): 1, (1, 0): 1, (0, 2): 2, (2, 0): 2, (1, 1): 3, (1, 2): 4, (2, 1): 4, (2, 2): 5}


def iota(shape, axis):
    return lax.broadcasted_iota(jnp.int32, shape, axis)


def split(x):
    hi = x.astype(BF16)
    return hi, (x - hi.astype(F32)).astype(BF16)


def mm(a, b):
    return lax.dot_general(a, b, (((1,), (0,)), ((), ())), preferred_element_type=F32)


def mm_exact(a, b, transposed=False):
    dims = (((1,), (1 if transposed else 0,)), ((), ()))
    return lax.dot_general(a, b, dims, precision=HIGHEST, preferred_element_type=F32)


def solve(corr, gram):
    m = jnp.concatenate([corr, gram], axis=0)
    shape = (32, 16)
    lane = iota(shape, 1)
    wide = [jnp.broadcast_to(m[:, j : j + 1], shape) for j in range(16)]
    for j in range(16):
        col = wide[j] / jnp.broadcast_to(wide[j][j : j + 1, :], shape)
        m = jnp.where(lane == j, col, m - col * jnp.broadcast_to(m[j : j + 1, :], shape))
        for n in range(j + 1, 16):
            wide[n] = wide[n] - col * jnp.broadcast_to(wide[n][j : j + 1, :], shape)
    return m[16:32, :]


def finish(scale, x_hbm, pq_hbm, z_hbm, next_ref, ray_ref, corr_ref, norm_ref, x_ref, pq_ref, z_ref, in_sem):
    gram_in = pltpu.make_async_copy(z_hbm, z_ref, in_sem.at[0])
    x_in = pltpu.make_async_copy(x_hbm, x_ref, in_sem.at[1])
    pq_in = pltpu.make_async_copy(pq_hbm, pq_ref, in_sem.at[2])
    for copy in (gram_in, x_in, pq_in):
        copy.start()
    gram_in.wait()
    packed = jnp.concatenate([z_ref[:, 0:64], z_ref[:, 64:128]], axis=0)
    xp, pq, mix = (packed[:, 16 * i : 16 * i + 16] for i in range(3))
    qq = packed[:, 49:50]
    flipped = jnp.transpose(mix)
    row, col = iota((16, 16), 0), iota((16, 16), 1)
    eye = row == col
    xx = jnp.where(col <= row, mix, flipped)
    pp = jnp.where(eye, packed[:, 48:49], jnp.where(col > row, mix, flipped))
    one = jnp.where(eye, 1.0, 0.0).astype(F32)
    c0 = solve(xx, xp)
    at = one + STEP * c0
    left = mm_exact(at, jnp.concatenate([xx, xp, pp, pq], axis=1))
    a_xx, a_xp, a_pp, a_pq = (left[:, 16 * i : 16 * i + 16] for i in range(4))
    y1, y2, y3 = a_xx - STEP * xp, a_xp - STEP * pp, a_pp - STEP * pq
    right = mm_exact(jnp.concatenate([y1, y2], axis=0), at, transposed=True)
    corr = right[0:16] - STEP * y2
    gram = right[16:32] - STEP * y3
    c1 = solve(corr, gram)

    both = c0 + c1
    factor = jnp.concatenate([STEP * both + STEP * STEP * mm_exact(c1, c0), -STEP * STEP * both], axis=1)
    f_hi, f_lo = split(factor)
    x_in.wait()
    pq_in.wait()
    for r in range(4):
        for d in range(3):
            rows, lanes = slice(d * 16, (d + 1) * 16), slice(r * 128, (r + 1) * 128)
            x, p, q = x_ref[rows, lanes], pq_ref[0, r, rows, :], pq_ref[1, r, rows, :]
            hi, lo = split(jnp.concatenate([x, p], axis=0))
            moved = mm(f_hi, hi) + mm(f_lo, hi) + mm(f_hi, lo)
            next_ref[rows, lanes] = (x - 2.0 * STEP * p) + (moved + STEP * STEP * q)

    corr_ref[...] = corr * scale
    ray_ref[...] = gram * scale
    squares = jnp.sum(a_pp * at - 2.0 * STEP * jnp.where(eye, a_pq, 0.0), axis=1, keepdims=True) + STEP * STEP * qq
    norms = (squares - jnp.sum(gram * c1, axis=1, keepdims=True)) * scale
    norm_ref[...] = jnp.sum(jnp.where(eye, norms, 0.0), axis=0, keepdims=True)


def kernel(
    ny, nz,
    x_hbm, pos_hbm, pairs_hbm, count_hbm,
    pq_hbm, z_hbm,
    pos_ref, pairs_ref, count_ref, in_sem, z_ref, out_sem,
    xg, pg, qg, shi, slo, lw, dacc, pay, ra, rb, rc,
    halo_send, halo_recv, p_send, p_recv, q_send, q_recv, a_send, a_recv, b_send, b_recv, c_send, c_recv,
):
    ty, tz, core, col = (lax.axis_index(n) for n in ("ty", "tz", "core", "col"))
    tiles = ny * nz * 2
    t = (ty * nz + tz) * 2 + core
    low = col < 2

    def at_tile(index, c):
        return (lax.div(index, 2 * nz), lax.rem(lax.div(index, 2), nz), lax.rem(index, 2), c)

    after, before = lax.rem(t + 1, tiles), lax.rem(t + tiles - 1, tiles)
    across = jnp.where(low, before, after)
    across_cols = (jnp.where(low, 2, 0), jnp.where(low, 3, 1))

    fetches = [
        pltpu.make_async_copy(count_hbm, count_ref, in_sem.at[0]),
        pltpu.make_async_copy(pairs_hbm, pairs_ref, in_sem.at[1]),
        pltpu.make_async_copy(pos_hbm, pos_ref, in_sem.at[2]),
    ]
    for r in range(4):
        lanes = slice(r * 128, (r + 1) * 128)
        fetches.append(pltpu.make_async_copy(x_hbm.at[:, lanes], xg.at[2 + r, 0:48, :], in_sem.at[3 + r]))
    for fetch in fetches:
        fetch.start()

    barrier = pltpu.get_barrier_semaphore()

    def greet(where):
        pl.semaphore_signal(barrier, inc=1, device_id=where, device_id_type=MESH)

    @pl.when(core == 1)
    def _():
        for o in range(1, ny):
            greet((lax.rem(ty + o, ny), tz, core, col))
        for o in range(1, nz):
            greet((ty, lax.rem(tz + o, nz), core, col))

    @pl.when(core == 0)
    def _():
        for o in range(1, nz):
            greet((ty, lax.rem(tz + o, nz), 1, col))

    for c in across_cols:
        greet(at_tile(across, c))
    greet(at_tile(after, col))
    greet(at_tile(before, col))
    for o in range(1, 4):
        greet((ty, tz, core, lax.rem(col + o, 4)))
        greet((ty, tz, 1 - core, lax.rem(col + o, 4)))
    greet((ty, tz, 1 - core, col))

    for fetch in fetches:
        fetch.wait()
    lane = iota((1, 128), 1)
    rows, cols = pairs_ref[0], pairs_ref[1]
    slot_col = iota((4, 8), 0)
    counts = jnp.zeros((4, 8), jnp.int32)
    for c in range(4):
        counts = jnp.where(slot_col == c, count_ref[:, c : c + 1], counts)
    live = jnp.where(iota((4, 8), 1) < counts, 1.0, 0.0).astype(F32)
    reach = cols - t * 4 - rows
    for r in range(4):
        xg[2 + r, 48:56, :] = jnp.zeros((8, 128), F32)
        xg[2 + r, 48:51, :] = pos_ref[:, r * 128 : (r + 1) * 128]
        listed = jnp.zeros((1, 128), F32)
        for k in range(3):
            here = jnp.where((rows == r) & (reach == k), live, 0.0)
            total = jnp.sum(jnp.sum(here, axis=1, keepdims=True), axis=0, keepdims=True)
            listed = jnp.where(lane == k, total, listed)
        xg[2 + r, 51:52, :] = listed

    dacc[...] = jnp.zeros_like(dacc)
    pay[...] = jnp.zeros_like(pay)
    own = 2 + col

    def spring_block(q, slot):
        mine = [xg[own, 48 + d : 49 + d, :] for d in range(3)]
        listed = xg[jnp.minimum(slot, own), 51:52, :]
        times = jnp.sum(jnp.where(lane == jnp.abs(slot - own), listed, 0.0), axis=1, keepdims=True)
        times = times * (1.0 / 64.0)
        near = jnp.transpose(xg[slot, 48:56, :])
        sums = [dacc[m] for m in range(6)]
        for ch in range(4):
            part = near[ch * 32 : (ch + 1) * 32]
            off = [part[:, d : d + 1] - mine[d] for d in range(3)]
            dist = off[0] * off[0] + off[1] * off[1] + off[2] * off[2]
            fall = 1.0 - dist * (1.0 / 225.0)
            weight = jnp.where(dist < 225.0, fall * fall, 0.0) * times / jnp.maximum(dist, 1.0)
            by = [weight * o for o in off]
            at = pl.ds(pl.multiple_of(q * 128 + ch * 32, 32), 32)
            for m, (c, d) in enumerate(MATS):
                s = by[c] * off[d]
                hi, lo = split(s)
                shi[at, m * 128 : (m + 1) * 128] = hi
                slo[at, m * 128 : (m + 1) * 128] = lo
                sums[m] = sums[m] + ((s[0:8] + s[8:16]) + (s[16:24] + s[24:32]))
        for m in range(6):
            dacc[m] = sums[m]

    first = jnp.where(low, 2, 3)
    late = (
        jnp.where(col == 0, 0, jnp.where(col == 1, 1, jnp.where(col == 2, 2, 6))),
        jnp.where(col == 0, 1, jnp.where(col == 1, 5, jnp.where(col == 2, 6, 7))),
    )
    slots = (first, first + 1, first + 2) + late

    pl.semaphore_wait(barrier, 11 + core * (ny + 2 * nz - 3))
    from_slot, to_slot = jnp.where(low, 4, 2), jnp.where(low, 0, 6)
    halo = pltpu.make_async_remote_copy(
        src_ref=xg.at[pl.ds(from_slot, 2)],
        dst_ref=xg.at[pl.ds(to_slot, 2)],
        send_sem=halo_send,
        recv_sem=halo_recv,
        device_id=at_tile(jnp.where(low, after, before), col),
        device_id_type=MESH,
    )
    halo.start()

    def near_vectors(source, q):
        hi, lo = split(source[slots[q], 0:48, :])
        lw[0:48, q * 128 : (q + 1) * 128] = hi
        lw[48:96, q * 128 : (q + 1) * 128] = lo

    def near_sum(start, stop):
        a, b = start * 128, stop * 128
        both = mm(lw[:, a:b], shi[a:b, :])
        return both[0:48] + both[48:96] + mm(lw[0:48, a:b], slo[a:b, :])

    def first_blocks(q, carry):
        spring_block(q, first + q)
        return carry

    lax.fori_loop(0, 3, first_blocks, 0)
    for q in range(3):
        near_vectors(xg, q)
    gathered = near_sum(0, 3)
    halo.wait_recv()

    def late_blocks(q, carry):
        spring_block(3 + q, jnp.where(q == 0, late[0], late[1]))
        return carry

    lax.fori_loop(0, 2, late_blocks, 0)
    for q in range(3, 5):
        near_vectors(xg, q)
    gathered = gathered + near_sum(3, 5)
    diag = [jnp.sum(dacc[m], axis=0, keepdims=True) for m in range(6)]

    def finish_product(gathered, source):
        here = [source[own, d * 16 : (d + 1) * 16, :] for d in range(3)]
        out = []
        for c in range(3):
            acc = None
            for d in range(3):
                m = MAT_OF[(c, d)]
                term = diag[m] * here[d] - gathered[d * 16 : (d + 1) * 16, m * 128 : (m + 1) * 128]
                acc = term if acc is None else acc + term
            out.append(acc)
        return here, out

    def moved(buf, at, send, recv, where):
        return pltpu.make_async_remote_copy(
            src_ref=buf.at[at], dst_ref=buf.at[at], send_sem=send, recv_sem=recv, device_id=where, device_id_type=MESH
        )

    here, first_product = finish_product(gathered, xg)
    for d in range(3):
        pg[own, d * 16 : (d + 1) * 16, :] = first_product[d]
    edge = jnp.logical_or(col == 0, col == 3)

    def across_copy(n, c):
        slot = jnp.where(low, 6 + col, col - 2)
        return pltpu.make_async_remote_copy(
            src_ref=pg.at[own], dst_ref=pg.at[slot], send_sem=p_send.at[n], recv_sem=p_recv.at[slot],
            device_id=at_tile(across, c), device_id_type=MESH,
        )

    def line_copy(o):
        return moved(pg, own, p_send.at[1 + o], p_recv.at[own], (ty, tz, core, lax.rem(col + o, 4)))

    def rest_copy(o):
        return moved(qg, col, q_send.at[o - 1], q_recv.at[col], (ty, tz, core, lax.rem(col + o, 4)))

    near_across = across_copy(0, jnp.where(low, 3, 0))
    next_across = across_copy(1, jnp.where(low, 2, 1))

    def is_far(o):
        return jnp.logical_and(edge, lax.rem(col + o, 4) == 3 - col)

    near_across.start()

    @pl.when(edge)
    def _():
        next_across.start()

    for o in (2, 1, 3):
        @pl.when(jnp.logical_not(is_far(o)))
        def _():
            line_copy(o).start()

    def arrived(buf, slot, recv):
        moved(buf, slot, p_send.at[0], recv, (ty, tz, core, lax.rem(col + 1, 4))).wait_recv()

    for o in range(1, 4):
        other = 2 + lax.rem(col + o, 4)

        @pl.when(jnp.logical_not(is_far(o)))
        def _():
            arrived(pg, other, p_recv.at[other])

    near_slot = jnp.where(low, 1, 6)
    arrived(pg, near_slot, p_recv.at[near_slot])

    @pl.when(edge)
    def _():
        next_slot = jnp.where(low, 0, 7)
        arrived(pg, next_slot, p_recv.at[next_slot])

    for q in range(5):
        near_vectors(pg, q)
    _, second_product = finish_product(near_sum(0, 5), pg)

    for d in range(3):
        qg[col, d * 16 : (d + 1) * 16, :] = second_product[d]
    x, p, q = (jnp.concatenate(parts, axis=1) for parts in (here, first_product, second_product))
    z_x = mm_exact(jnp.concatenate([x, p], axis=0), x, transposed=True)
    z_p = mm_exact(p, jnp.concatenate([p, q], axis=0), transposed=True)
    mix = jnp.where(iota((16, 16), 1) <= iota((16, 16), 0), z_x[0:16], z_p[:, 0:16])
    p_sq, q_sq = (jnp.sum(v * v, axis=1, keepdims=True) for v in (p, q))
    for h in range(2):
        rows, at = slice(8 * h, 8 * h + 8), 64 * h
        pay[:, at : at + 16] = z_x[16:32][rows]
        pay[:, at + 16 : at + 32] = z_p[rows, 16:32]
        pay[:, at + 32 : at + 48] = mix[rows]
        pay[:, at + 48 : at + 49] = p_sq[rows]
        pay[:, at + 49 : at + 50] = q_sq[rows]

    line = col * 2 + core

    def to_line(x):
        return pltpu.make_async_remote_copy(
            src_ref=pay, dst_ref=ra.at[line], send_sem=a_send.at[x], recv_sem=a_recv.at[line],
            device_id=(ty, tz, 1, x), device_id_type=MESH,
        )

    for x in range(4):
        @pl.when(jnp.logical_or(core == 0, col != x))
        def _():
            to_line(x).start()

    def summed(buf, n):
        parts = [buf[i] for i in range(n)]
        while len(parts) > 1:
            parts = [a + b for a, b in zip(parts[0::2], parts[1::2])] + parts[len(parts) & ~1 :]
        return parts[0]

    def far_first(n):
        return sorted(range(1, n), key=lambda o: -min(o, n - o))

    products_out = (
        pltpu.make_async_copy(pg.at[2:6], pq_hbm.at[0], out_sem.at[1]),
        pltpu.make_async_copy(qg, pq_hbm.at[1], out_sem.at[2]),
    )

    def put_products():
        for o in range(1, 4):
            rest_copy(o).start()

            @pl.when(is_far(o))
            def _():
                line_copy(o).start()

        for o in range(1, 4):
            other = lax.rem(col + o, 4)
            arrived(qg, other, q_recv.at[other])

            @pl.when(is_far(o))
            def _():
                arrived(pg, 2 + other, p_recv.at[2 + other])

        for copy in products_out:
            copy.start()

    @pl.when(core == 1)
    def _():
        ra[line] = pay[...]
        for o in range(1, 8):
            other = lax.rem(line + o, 8)
            moved(ra, other, a_send.at[0], a_recv.at[other], (ty, tz, 0, col)).wait_recv()
        rb[ty] = summed(ra, 8)
        done = []
        for o in far_first(ny):
            done.append(moved(rb, ty, b_send.at[o], b_recv.at[ty], (lax.rem(ty + o, ny), tz, 1, col)))
            done[-1].start()
        put_products()
        for o in range(1, ny):
            other = lax.rem(ty + o, ny)
            moved(rb, other, b_send.at[o], b_recv.at[other], (other, tz, 1, col)).wait_recv()
        rc[tz] = summed(rb, ny)
        for o in far_first(nz) + [0]:
            place = lax.rem(tz + o, nz)
            done.append(moved(rc, tz, c_send.at[0, o], c_recv.at[tz], (ty, place, 0, col)))
            done[-1].start()
            if o:
                done.append(moved(rc, tz, c_send.at[1, o], c_recv.at[tz], (ty, place, 1, col)))
                done[-1].start()
        for o in range(1, nz):
            other = lax.rem(tz + o, nz)
            moved(rc, other, c_send.at[0, 0], c_recv.at[other], (ty, tz, 0, col)).wait_recv()
        for copy in done:
            copy.wait_send()
        for x in range(4):
            @pl.when(col != x)
            def _():
                to_line(x).wait_send()

    @pl.when(core == 0)
    def _():
        for x in range(4):
            to_line(x).wait_send()
        put_products()
        for other in range(nz):
            moved(rc, other, c_send.at[0, 0], c_recv.at[other], (ty, tz, 1, col)).wait_recv()

    z_ref[...] = summed(rc, nz)
    gram_out = pltpu.make_async_copy(z_ref, z_hbm, out_sem.at[0])
    gram_out.start()
    near_across.wait_send()

    @pl.when(edge)
    def _():
        next_across.wait_send()

    for o in range(1, 4):
        line_copy(o).wait_send()
        rest_copy(o).wait_send()
    halo.wait_send()
    gram_out.wait()
    for copy in products_out:
        copy.wait()


def per_device(ny, nz, positions, trial_block, pair_tiles, pair_count):
    scale = 1.0 / (3.0 * ny * nz * 2 * 512)
    vmem = pl.BlockSpec(memory_space=pltpu.VMEM)
    dma = pltpu.SemaphoreType.DMA
    hbm = pl.BlockSpec(memory_space=pltpu.HBM)
    block = trial_block.reshape(48, 512)
    products, gram = pl.pallas_call(
        functools.partial(kernel, ny, nz),
        out_shape=(jax.ShapeDtypeStruct((2, 4, 48, 128), F32), jax.ShapeDtypeStruct((8, 128), F32)),
        in_specs=[hbm] * 4,
        out_specs=(hbm, hbm),
        scratch_shapes=[
            pltpu.VMEM((3, 512), F32),
            pltpu.VMEM((2, 4, 8), jnp.int32),
            pltpu.VMEM((1, 4), jnp.int32),
            dma((7,)),
            pltpu.VMEM((8, 128), F32),
            dma((3,)),
            pltpu.VMEM((8, 56, 128), F32),
            pltpu.VMEM((8, 48, 128), F32),
            pltpu.VMEM((4, 48, 128), F32),
            pltpu.VMEM((640, 768), BF16),
            pltpu.VMEM((640, 768), BF16),
            pltpu.VMEM((96, 640), BF16),
            pltpu.VMEM((6, 8, 128), F32),
            pltpu.VMEM((8, 128), F32),
            pltpu.VMEM((8, 8, 128), F32),
            pltpu.VMEM((ny, 8, 128), F32),
            pltpu.VMEM((nz, 8, 128), F32),
            dma, dma,
            dma((5,)), dma((8,)),
            dma((3,)), dma((4,)),
            dma((4,)), dma((8,)),
            dma((ny,)), dma((ny,)),
            dma((2, nz)), dma((nz,)),
        ],
        compiler_params=pltpu.CompilerParams(collective_id=0, has_side_effects=True, vmem_limit_bytes=60 * 1024 * 1024),
        name="gram_blocks",
    )(block, positions, pair_tiles.reshape(2, 4, 8), pair_count)
    block, rayleigh, correlation, norms = pl.pallas_call(
        functools.partial(finish, scale),
        out_shape=(
            jax.ShapeDtypeStruct((48, 512), F32),
            jax.ShapeDtypeStruct((16, 16), F32),
            jax.ShapeDtypeStruct((16, 16), F32),
            jax.ShapeDtypeStruct((1, 16), F32),
        ),
        in_specs=[hbm] * 3,
        out_specs=(vmem,) * 4,
        scratch_shapes=[pltpu.VMEM((48, 512), F32), pltpu.VMEM((2, 4, 48, 128), F32), pltpu.VMEM((8, 128), F32), dma((3,))],
        compiler_params=pltpu.CompilerParams(vmem_limit_bytes=60 * 1024 * 1024),
        name="finish",
    )(block, products, gram)
    return block.reshape(3, 16, 512), rayleigh, correlation, norms.reshape(16)


def build(finer):
    return jax.shard_map(
        functools.partial(per_device, finer.shape["ty"], finer.shape["tz"]),
        mesh=finer,
        in_specs=(P(None, TILE), P(None, None, TILE), P(None, TILE, None, None), P(TILE, None)),
        out_specs=(P(None, None, TILE), P(), P(), P()),
        check_vma=False,
    )


def solution(mesh):
    return build(Mesh(mesh.devices.reshape(8, 8, 2, mesh.shape["col"]), (*TILE, "col")))
```

```python
import functools

import jax
import jax.numpy as jnp
from jax import lax
from jax.experimental import pallas as pl
from jax.experimental.pallas import tpu as pltpu
from jax.sharding import Mesh
from jax.sharding import PartitionSpec as P

TILE = ("ty", "tz", "core")
MESH = pl.DeviceIdType.MESH
F32 = jnp.float32
BF16 = jnp.bfloat16
HIGHEST = lax.Precision.HIGHEST

STEP = 0.2
MATS = ((0, 0), (0, 1), (0, 2), (1, 1), (1, 2), (2, 2))
MAT_OF = {(0, 0): 0, (0, 1): 1, (1, 0): 1, (0, 2): 2, (2, 0): 2, (1, 1): 3, (1, 2): 4, (2, 1): 4, (2, 2): 5}


def iota(shape, axis):
    return lax.broadcasted_iota(jnp.int32, shape, axis)


def split(x):
    hi = x.astype(BF16)
    return hi, (x - hi.astype(F32)).astype(BF16)


def mm(a, b):
    return lax.dot_general(a, b, (((1,), (0,)), ((), ())), preferred_element_type=F32)


def mm_exact(a, b, transposed=False):
    dims = (((1,), (1 if transposed else 0,)), ((), ()))
    return lax.dot_general(a, b, dims, precision=HIGHEST, preferred_element_type=F32)


def solve(corr, gram):
    m = jnp.concatenate([corr, gram], axis=0)
    shape = (32, 16)
    lane = iota(shape, 1)
    wide = [jnp.broadcast_to(m[:, j : j + 1], shape) for j in range(16)]
    for j in range(16):
        col = wide[j] / jnp.broadcast_to(wide[j][j : j + 1, :], shape)
        m = jnp.where(lane == j, col, m - col * jnp.broadcast_to(m[j : j + 1, :], shape))
        for n in range(j + 1, 16):
            wide[n] = wide[n] - col * jnp.broadcast_to(wide[n][j : j + 1, :], shape)
    return m[16:32, :]


def finish(scale, x_hbm, pq_hbm, z_hbm, next_ref, ray_ref, corr_ref, norm_ref, x_ref, pq_ref, z_ref, in_sem):
    gram_in = pltpu.make_async_copy(z_hbm, z_ref, in_sem.at[0])
    x_in = pltpu.make_async_copy(x_hbm, x_ref, in_sem.at[1])
    pq_in = pltpu.make_async_copy(pq_hbm, pq_ref, in_sem.at[2])
    for copy in (gram_in, x_in, pq_in):
        copy.start()
    gram_in.wait()
    packed = jnp.concatenate([z_ref[:, 0:64], z_ref[:, 64:128]], axis=0)
    xp, pq, mix = (packed[:, 16 * i : 16 * i + 16] for i in range(3))
    qq = packed[:, 49:50]
    flipped = jnp.transpose(mix)
    row, col = iota((16, 16), 0), iota((16, 16), 1)
    eye = row == col
    xx = jnp.where(col <= row, mix, flipped)
    pp = jnp.where(eye, packed[:, 48:49], jnp.where(col > row, mix, flipped))
    one = jnp.where(eye, 1.0, 0.0).astype(F32)
    c0 = solve(xx, xp)
    at = one + STEP * c0
    left = mm_exact(at, jnp.concatenate([xx, xp, pp, pq], axis=1))
    a_xx, a_xp, a_pp, a_pq = (left[:, 16 * i : 16 * i + 16] for i in range(4))
    y1, y2, y3 = a_xx - STEP * xp, a_xp - STEP * pp, a_pp - STEP * pq
    right = mm_exact(jnp.concatenate([y1, y2], axis=0), at, transposed=True)
    corr = right[0:16] - STEP * y2
    gram = right[16:32] - STEP * y3
    c1 = solve(corr, gram)

    both = c0 + c1
    factor = jnp.concatenate([STEP * both + STEP * STEP * mm_exact(c1, c0), -STEP * STEP * both], axis=1)
    f_hi, f_lo = split(factor)
    x_in.wait()
    pq_in.wait()
    for r in range(4):
        for d in range(3):
            rows, lanes = slice(d * 16, (d + 1) * 16), slice(r * 128, (r + 1) * 128)
            x, p, q = x_ref[rows, lanes], pq_ref[0, r, rows, :], pq_ref[1, r, rows, :]
            hi, lo = split(jnp.concatenate([x, p], axis=0))
            moved = mm(f_hi, hi) + mm(f_lo, hi) + mm(f_hi, lo)
            next_ref[rows, lanes] = (x - 2.0 * STEP * p) + (moved + STEP * STEP * q)

    corr_ref[...] = corr * scale
    ray_ref[...] = gram * scale
    squares = jnp.sum(a_pp * at - 2.0 * STEP * jnp.where(eye, a_pq, 0.0), axis=1, keepdims=True) + STEP * STEP * qq
    norms = (squares - jnp.sum(gram * c1, axis=1, keepdims=True)) * scale
    norm_ref[...] = jnp.sum(jnp.where(eye, norms, 0.0), axis=0, keepdims=True)


def kernel(
    ny, nz,
    x_hbm, pos_hbm, pairs_hbm, count_hbm,
    pq_hbm, z_hbm,
    pos_ref, pairs_ref, count_ref, in_sem, z_ref, out_sem,
    xg, pg, qg, shi, slo, lw, dacc, pay, ra, rb, rc,
    halo_send, halo_recv, p_send, p_recv, far_send, far_recv, q_send, q_recv, a_send, a_recv, b_send, b_recv, c_send, c_recv,
):
    ty, tz, core, col = (lax.axis_index(n) for n in ("ty", "tz", "core", "col"))
    tiles = ny * nz * 2
    t = (ty * nz + tz) * 2 + core
    low = col < 2

    def at_tile(index, c):
        return (lax.div(index, 2 * nz), lax.rem(lax.div(index, 2), nz), lax.rem(index, 2), c)

    after, before = lax.rem(t + 1, tiles), lax.rem(t + tiles - 1, tiles)
    across = jnp.where(low, before, after)
    across_cols = (jnp.where(low, 2, 0), jnp.where(low, 3, 1))

    fetches = [
        pltpu.make_async_copy(count_hbm, count_ref, in_sem.at[0]),
        pltpu.make_async_copy(pairs_hbm, pairs_ref, in_sem.at[1]),
        pltpu.make_async_copy(pos_hbm, pos_ref, in_sem.at[2]),
    ]
    for r in range(4):
        lanes = slice(r * 128, (r + 1) * 128)
        fetches.append(pltpu.make_async_copy(x_hbm.at[:, lanes], xg.at[2 + r, 0:48, :], in_sem.at[3]))
    for fetch in fetches:
        fetch.start()

    barrier = pltpu.get_barrier_semaphore()

    def greet(where):
        pl.semaphore_signal(barrier, inc=1, device_id=where, device_id_type=MESH)

    @pl.when(core == 1)
    def _():
        for o in range(1, ny):
            greet((lax.rem(ty + o, ny), tz, core, col))
        for o in range(1, nz):
            greet((ty, lax.rem(tz + o, nz), core, col))

    @pl.when(core == 0)
    def _():
        for o in range(1, nz):
            greet((ty, lax.rem(tz + o, nz), 1, col))

    for c in across_cols:
        greet(at_tile(across, c))
    greet(at_tile(after, col))
    greet(at_tile(before, col))
    for o in range(1, 4):
        greet((ty, tz, core, lax.rem(col + o, 4)))
        greet((ty, tz, 1 - core, lax.rem(col + o, 4)))
    greet((ty, tz, 1 - core, col))

    for fetch in fetches[:3]:
        fetch.wait()
    pltpu.make_async_copy(xg.at[2:6, 0:48, :], xg.at[2:6, 0:48, :], in_sem.at[3]).wait()
    lane = iota((1, 128), 1)
    rows, cols = pairs_ref[0], pairs_ref[1]
    slot_col = iota((4, 8), 0)
    counts = jnp.zeros((4, 8), jnp.int32)
    for c in range(4):
        counts = jnp.where(slot_col == c, count_ref[:, c : c + 1], counts)
    live = jnp.where(iota((4, 8), 1) < counts, 1.0, 0.0).astype(F32)
    reach = cols - t * 4 - rows
    for r in range(4):
        xg[2 + r, 48:56, :] = jnp.zeros((8, 128), F32)
        xg[2 + r, 48:51, :] = pos_ref[:, r * 128 : (r + 1) * 128]
        listed = jnp.zeros((1, 128), F32)
        for k in range(3):
            here = jnp.where((rows == r) & (reach == k), live, 0.0)
            total = jnp.sum(jnp.sum(here, axis=1, keepdims=True), axis=0, keepdims=True)
            listed = jnp.where(lane == k, total, listed)
        xg[2 + r, 51:52, :] = listed

    dacc[...] = jnp.zeros_like(dacc)
    pay[...] = jnp.zeros_like(pay)
    own = 2 + col

    def spring_block(q, slot):
        mine = [xg[own, 48 + d : 49 + d, :] for d in range(3)]
        listed = xg[jnp.minimum(slot, own), 51:52, :]
        times = jnp.sum(jnp.where(lane == jnp.abs(slot - own), listed, 0.0), axis=1, keepdims=True)
        times = times * (1.0 / 64.0)
        near = jnp.transpose(xg[slot, 48:56, :])
        sums = [dacc[m] for m in range(6)]
        for ch in range(4):
            part = near[ch * 32 : (ch + 1) * 32]
            off = [part[:, d : d + 1] - mine[d] for d in range(3)]
            dist = off[0] * off[0] + off[1] * off[1] + off[2] * off[2]
            fall = 1.0 - dist * (1.0 / 225.0)
            weight = jnp.where(dist < 225.0, fall * fall, 0.0) * times / jnp.maximum(dist, 1.0)
            by = [weight * o for o in off]
            at = pl.ds(pl.multiple_of(q * 128 + ch * 32, 32), 32)
            for m, (c, d) in enumerate(MATS):
                s = by[c] * off[d]
                hi, lo = split(s)
                shi[at, m * 128 : (m + 1) * 128] = hi
                slo[at, m * 128 : (m + 1) * 128] = lo
                sums[m] = sums[m] + ((s[0:8] + s[8:16]) + (s[16:24] + s[24:32]))
        for m in range(6):
            dacc[m] = sums[m]

    first = jnp.where(low, 2, 3)
    late = (
        jnp.where(col == 0, 0, jnp.where(col == 1, 1, jnp.where(col == 2, 2, 6))),
        jnp.where(col == 0, 1, jnp.where(col == 1, 5, jnp.where(col == 2, 6, 7))),
    )
    slots = (first, first + 1, first + 2) + late

    pl.semaphore_wait(barrier, 11 + core * (ny + 2 * nz - 3))
    from_slot, to_slot = jnp.where(low, 4, 2), jnp.where(low, 0, 6)

    def halo_copy(n, rows):
        return pltpu.make_async_remote_copy(
            src_ref=xg.at[pl.ds(from_slot, 2), rows],
            dst_ref=xg.at[pl.ds(to_slot, 2), rows],
            send_sem=halo_send.at[n],
            recv_sem=halo_recv.at[n],
            device_id=at_tile(jnp.where(low, after, before), col),
            device_id_type=MESH,
        )

    halo = (halo_copy(0, slice(48, 56)), halo_copy(1, slice(0, 48)))
    for copy in halo:
        copy.start()

    def near_vectors(source, q):
        hi, lo = split(source[slots[q], 0:48, :])
        lw[0:48, q * 128 : (q + 1) * 128] = hi
        lw[48:96, q * 128 : (q + 1) * 128] = lo

    def near_sum(start, stop):
        a, b = start * 128, stop * 128
        both = mm(lw[:, a:b], shi[a:b, :])
        return both[0:48] + both[48:96] + mm(lw[0:48, a:b], slo[a:b, :])

    def first_blocks(q, carry):
        spring_block(q, first + q)
        return carry

    lax.fori_loop(0, 3, first_blocks, 0)
    for q in range(3):
        near_vectors(xg, q)
    gathered = near_sum(0, 3)
    halo[0].wait_recv()

    def late_blocks(q, carry):
        spring_block(3 + q, jnp.where(q == 0, late[0], late[1]))
        return carry

    lax.fori_loop(0, 2, late_blocks, 0)
    halo[1].wait_recv()
    for q in range(3, 5):
        near_vectors(xg, q)
    gathered = gathered + near_sum(3, 5)
    diag = [jnp.sum(dacc[m], axis=0, keepdims=True) for m in range(6)]

    def finish_product(gathered, source):
        here = [source[own, d * 16 : (d + 1) * 16, :] for d in range(3)]
        out = []
        for c in range(3):
            acc = None
            for d in range(3):
                m = MAT_OF[(c, d)]
                term = diag[m] * here[d] - gathered[d * 16 : (d + 1) * 16, m * 128 : (m + 1) * 128]
                acc = term if acc is None else acc + term
            out.append(acc)
        return here, out

    def all_sent(buf, send):
        moved(buf, slice(None), send, q_recv, (ty, tz, 1 - core, col)).wait_send()

    def all_here(buf, recv):
        moved(buf, slice(None), q_send, recv, (ty, tz, 1 - core, col)).wait_recv()

    def moved(buf, at, send, recv, where):
        return pltpu.make_async_remote_copy(
            src_ref=buf.at[at], dst_ref=buf.at[at], send_sem=send, recv_sem=recv, device_id=where, device_id_type=MESH
        )

    here, first_product = finish_product(gathered, xg)
    for d in range(3):
        pg[own, d * 16 : (d + 1) * 16, :] = first_product[d]
    edge = jnp.logical_or(col == 0, col == 3)

    def across_copy(c):
        slot = jnp.where(low, 6 + col, col - 2)
        return pltpu.make_async_remote_copy(
            src_ref=pg.at[own], dst_ref=pg.at[slot], send_sem=p_send, recv_sem=p_recv,
            device_id=at_tile(across, c), device_id_type=MESH,
        )

    def line_copy(o, send, recv):
        return moved(pg, own, send, recv, (ty, tz, core, lax.rem(col + o, 4)))

    def rest_copy(o):
        return moved(qg, col, q_send, q_recv, (ty, tz, core, lax.rem(col + o, 4)))

    near_across = across_copy(jnp.where(low, 3, 0))
    next_across = across_copy(jnp.where(low, 2, 1))

    def is_far(o):
        return jnp.logical_and(edge, lax.rem(col + o, 4) == 3 - col)

    near_across.start()

    @pl.when(edge)
    def _():
        next_across.start()

    for o in (2, 1, 3):
        @pl.when(jnp.logical_not(is_far(o)))
        def _():
            line_copy(o, p_send, p_recv).start()

    all_here(pg.at[0:4], p_recv)

    for q in range(5):
        near_vectors(pg, q)
    _, second_product = finish_product(near_sum(0, 5), pg)

    for d in range(3):
        qg[col, d * 16 : (d + 1) * 16, :] = second_product[d]
    x, p, q = (jnp.concatenate(parts, axis=1) for parts in (here, first_product, second_product))
    z_x = mm_exact(jnp.concatenate([x, p], axis=0), x, transposed=True)
    z_p = mm_exact(p, jnp.concatenate([p, q], axis=0), transposed=True)
    mix = jnp.where(iota((16, 16), 1) <= iota((16, 16), 0), z_x[0:16], z_p[:, 0:16])
    p_sq, q_sq = (jnp.sum(v * v, axis=1, keepdims=True) for v in (p, q))
    for h in range(2):
        rows, at = slice(8 * h, 8 * h + 8), 64 * h
        pay[:, at : at + 16] = z_x[16:32][rows]
        pay[:, at + 16 : at + 32] = z_p[rows, 16:32]
        pay[:, at + 32 : at + 48] = mix[rows]
        pay[:, at + 48 : at + 49] = p_sq[rows]
        pay[:, at + 49 : at + 50] = q_sq[rows]

    line = col * 2 + core

    def to_line(x):
        return pltpu.make_async_remote_copy(
            src_ref=pay, dst_ref=ra.at[line], send_sem=a_send, recv_sem=a_recv,
            device_id=(ty, tz, 1, x), device_id_type=MESH,
        )

    for x in range(4):
        @pl.when(jnp.logical_or(core == 0, col != x))
        def _():
            to_line(x).start()

    def y_copy(o):
        return moved(rb, ty, b_send, b_recv, (lax.rem(ty + o, ny), tz, 1, col))

    def z_copy(o, c):
        return moved(rc, tz, c_send.at[c], c_recv, (ty, lax.rem(tz + o, nz), c, col))

    def summed(buf, n):
        parts = [buf[i] for i in range(n)]
        while len(parts) > 1:
            parts = [a + b for a, b in zip(parts[0::2], parts[1::2])] + parts[len(parts) & ~1 :]
        return parts[0]

    def far_first(n):
        return sorted(range(1, n), key=lambda o: -min(o, n - o))

    products_out = (
        pltpu.make_async_copy(pg.at[2:6], pq_hbm.at[0], out_sem.at[1]),
        pltpu.make_async_copy(qg, pq_hbm.at[1], out_sem.at[2]),
    )

    def put_products():
        for o in range(1, 4):
            rest_copy(o).start()

            @pl.when(is_far(o))
            def _():
                line_copy(o, far_send, far_recv).start()

        all_here(qg.at[0:3], q_recv)

        @pl.when(edge)
        def _():
            all_here(pg.at[0], far_recv)

        for copy in products_out:
            copy.start()

    @pl.when(core == 1)
    def _():
        ra[line] = pay[...]
        all_here(ra.at[0:7], a_recv)
        rb[ty] = summed(ra, 8)
        for o in far_first(ny):
            y_copy(o).start()
        put_products()
        all_here(rb.at[0 : ny - 1], b_recv)
        rc[tz] = summed(rb, ny)
        for o in far_first(nz) + [0]:
            z_copy(o, 0).start()
            if o:
                z_copy(o, 1).start()
        all_here(rc.at[0 : nz - 1], c_recv)

    @pl.when(core == 0)
    def _():
        all_sent(ra.at[0:4], a_send)
        put_products()
        all_here(rc, c_recv)

    z_ref[...] = summed(rc, nz)
    gram_out = pltpu.make_async_copy(z_ref, z_hbm, out_sem.at[0])
    gram_out.start()

    @pl.when(core == 1)
    def _():
        all_sent(ra.at[0:3], a_send)
        all_sent(rb.at[0 : ny - 1], b_send)
        all_sent(rc, c_send.at[0])
        all_sent(rc.at[0 : nz - 1], c_send.at[1])

    all_sent(pg.at[0:4], p_send)
    all_sent(qg.at[0:3], q_send)

    @pl.when(edge)
    def _():
        all_sent(pg.at[0], far_send)

    for copy in halo:
        copy.wait_send()
    gram_out.wait()
    for copy in products_out:
        copy.wait()


def per_device(ny, nz, positions, trial_block, pair_tiles, pair_count):
    scale = 1.0 / (3.0 * ny * nz * 2 * 512)
    vmem = pl.BlockSpec(memory_space=pltpu.VMEM)
    dma = pltpu.SemaphoreType.DMA
    hbm = pl.BlockSpec(memory_space=pltpu.HBM)
    block = trial_block.reshape(48, 512)
    products, gram = pl.pallas_call(
        functools.partial(kernel, ny, nz),
        out_shape=(jax.ShapeDtypeStruct((2, 4, 48, 128), F32), jax.ShapeDtypeStruct((8, 128), F32)),
        in_specs=[hbm] * 4,
        out_specs=(hbm, hbm),
        scratch_shapes=[
            pltpu.VMEM((3, 512), F32),
            pltpu.VMEM((2, 4, 8), jnp.int32),
            pltpu.VMEM((1, 4), jnp.int32),
            dma((4,)),
            pltpu.VMEM((8, 128), F32),
            dma((3,)),
            pltpu.VMEM((8, 56, 128), F32),
            pltpu.VMEM((8, 48, 128), F32),
            pltpu.VMEM((4, 48, 128), F32),
            pltpu.VMEM((640, 768), BF16),
            pltpu.VMEM((640, 768), BF16),
            pltpu.VMEM((96, 640), BF16),
            pltpu.VMEM((6, 8, 128), F32),
            pltpu.VMEM((8, 128), F32),
            pltpu.VMEM((8, 8, 128), F32),
            pltpu.VMEM((ny, 8, 128), F32),
            pltpu.VMEM((nz, 8, 128), F32),
            dma((2,)), dma((2,)),
            dma, dma, dma, dma, dma, dma, dma, dma, dma, dma,
            dma((2,)), dma,
        ],
        compiler_params=pltpu.CompilerParams(collective_id=0, has_side_effects=True, vmem_limit_bytes=60 * 1024 * 1024),
        name="gram_blocks",
    )(block, positions, pair_tiles.reshape(2, 4, 8), pair_count)
    block, rayleigh, correlation, norms = pl.pallas_call(
        functools.partial(finish, scale),
        out_shape=(
            jax.ShapeDtypeStruct((48, 512), F32),
            jax.ShapeDtypeStruct((16, 16), F32),
            jax.ShapeDtypeStruct((16, 16), F32),
            jax.ShapeDtypeStruct((1, 16), F32),
        ),
        in_specs=[hbm] * 3,
        out_specs=(vmem,) * 4,
        scratch_shapes=[pltpu.VMEM((48, 512), F32), pltpu.VMEM((2, 4, 48, 128), F32), pltpu.VMEM((8, 128), F32), dma((3,))],
        compiler_params=pltpu.CompilerParams(vmem_limit_bytes=60 * 1024 * 1024),
        name="finish",
    )(block, products, gram)
    return block.reshape(3, 16, 512), rayleigh, correlation, norms.reshape(16)


def build(finer):
    return jax.shard_map(
        functools.partial(per_device, finer.shape["ty"], finer.shape["tz"]),
        mesh=finer,
        in_specs=(P(None, TILE), P(None, None, TILE), P(None, TILE, None, None), P(TILE, None)),
        out_specs=(P(None, None, TILE), P(), P(), P()),
        check_vma=False,
    )


def solution(mesh):
    return build(Mesh(mesh.devices.reshape(8, 8, 2, mesh.shape["col"]), (*TILE, "col")))
```

```python
import functools

import jax
import jax.numpy as jnp
from jax import lax
from jax.experimental import pallas as pl
from jax.experimental.pallas import tpu as pltpu
from jax.sharding import Mesh
from jax.sharding import PartitionSpec as P

TILE = ("ty", "tz", "core")
MESH = pl.DeviceIdType.MESH
F32 = jnp.float32
BF16 = jnp.bfloat16
HIGHEST = lax.Precision.HIGHEST

STEP = 0.2
MATS = ((0, 0), (0, 1), (0, 2), (1, 1), (1, 2), (2, 2))
MAT_OF = {(0, 0): 0, (0, 1): 1, (1, 0): 1, (0, 2): 2, (2, 0): 2, (1, 1): 3, (1, 2): 4, (2, 1): 4, (2, 2): 5}


def iota(shape, axis):
    return lax.broadcasted_iota(jnp.int32, shape, axis)


def split(x):
    hi = x.astype(BF16)
    return hi, (x - hi.astype(F32)).astype(BF16)


def mm(a, b):
    return lax.dot_general(a, b, (((1,), (0,)), ((), ())), preferred_element_type=F32)


def mm_exact(a, b, transposed=False):
    dims = (((1,), (1 if transposed else 0,)), ((), ()))
    return lax.dot_general(a, b, dims, precision=HIGHEST, preferred_element_type=F32)


def solve(corr, gram):
    m = jnp.concatenate([corr, gram], axis=0)
    shape = (32, 16)
    lane = iota(shape, 1)
    wide = [jnp.broadcast_to(m[:, j : j + 1], shape) for j in range(16)]
    for j in range(16):
        col = wide[j] / jnp.broadcast_to(wide[j][j : j + 1, :], shape)
        m = jnp.where(lane == j, col, m - col * jnp.broadcast_to(m[j : j + 1, :], shape))
        for n in range(j + 1, 16):
            wide[n] = wide[n] - col * jnp.broadcast_to(wide[n][j : j + 1, :], shape)
    return m[16:32, :]


def finish(scale, x_hbm, pq_hbm, z_hbm, next_ref, ray_ref, corr_ref, norm_ref, x_ref, pq_ref, z_ref, in_sem):
    gram_in = pltpu.make_async_copy(z_hbm, z_ref, in_sem.at[0])
    x_in = pltpu.make_async_copy(x_hbm, x_ref, in_sem.at[1])
    pq_in = pltpu.make_async_copy(pq_hbm, pq_ref, in_sem.at[2])
    for copy in (gram_in, x_in, pq_in):
        copy.start()
    gram_in.wait()
    packed = jnp.concatenate([z_ref[:, 0:64], z_ref[:, 64:128]], axis=0)
    xp, pq, mix = (packed[:, 16 * i : 16 * i + 16] for i in range(3))
    qq = packed[:, 49:50]
    flipped = jnp.transpose(mix)
    row, col = iota((16, 16), 0), iota((16, 16), 1)
    eye = row == col
    xx = jnp.where(col <= row, mix, flipped)
    pp = jnp.where(eye, packed[:, 48:49], jnp.where(col > row, mix, flipped))
    one = jnp.where(eye, 1.0, 0.0).astype(F32)
    c0 = solve(xx, xp)
    at = one + STEP * c0
    left = mm_exact(at, jnp.concatenate([xx, xp, pp, pq], axis=1))
    a_xx, a_xp, a_pp, a_pq = (left[:, 16 * i : 16 * i + 16] for i in range(4))
    y1, y2, y3 = a_xx - STEP * xp, a_xp - STEP * pp, a_pp - STEP * pq
    right = mm_exact(jnp.concatenate([y1, y2], axis=0), at, transposed=True)
    corr = right[0:16] - STEP * y2
    gram = right[16:32] - STEP * y3
    c1 = solve(corr, gram)

    both = c0 + c1
    factor = jnp.concatenate([STEP * both + STEP * STEP * mm_exact(c1, c0), -STEP * STEP * both], axis=1)
    f_hi, f_lo = split(factor)
    x_in.wait()
    pq_in.wait()
    for r in range(4):
        for d in range(3):
            rows, lanes = slice(d * 16, (d + 1) * 16), slice(r * 128, (r + 1) * 128)
            x, p, q = x_ref[rows, lanes], pq_ref[0, r, rows, :], pq_ref[1, r, rows, :]
            hi, lo = split(jnp.concatenate([x, p], axis=0))
            moved = mm(f_hi, hi) + mm(f_lo, hi) + mm(f_hi, lo)
            next_ref[rows, lanes] = (x - 2.0 * STEP * p) + (moved + STEP * STEP * q)

    corr_ref[...] = corr * scale
    ray_ref[...] = gram * scale
    squares = jnp.sum(a_pp * at - 2.0 * STEP * jnp.where(eye, a_pq, 0.0), axis=1, keepdims=True) + STEP * STEP * qq
    norms = (squares - jnp.sum(gram * c1, axis=1, keepdims=True)) * scale
    norm_ref[...] = jnp.sum(jnp.where(eye, norms, 0.0), axis=0, keepdims=True)


def kernel(
    ny, nz,
    x_hbm, pos_hbm, pairs_hbm, count_hbm,
    pq_hbm, z_hbm,
    pos_ref, pairs_ref, count_ref, in_sem, z_ref, out_sem,
    xg, pg, qg, shi, slo, lw, dacc, pay, ra, rb, rc,
    halo_send, halo_recv, p_send, p_recv, far_send, far_recv, q_send, q_recv, a_send, a_recv, b_send, b_recv, c_send, c_recv,
):
    ty, tz, core, col = (lax.axis_index(n) for n in ("ty", "tz", "core", "col"))
    tiles = ny * nz * 2
    t = (ty * nz + tz) * 2 + core
    low = col < 2

    def at_tile(index, c):
        return (lax.div(index, 2 * nz), lax.rem(lax.div(index, 2), nz), lax.rem(index, 2), c)

    after, before = lax.rem(t + 1, tiles), lax.rem(t + tiles - 1, tiles)
    across = jnp.where(low, before, after)
    across_cols = (jnp.where(low, 2, 0), jnp.where(low, 3, 1))

    fetches = [
        pltpu.make_async_copy(count_hbm, count_ref, in_sem.at[0]),
        pltpu.make_async_copy(pairs_hbm, pairs_ref, in_sem.at[1]),
        pltpu.make_async_copy(pos_hbm, pos_ref, in_sem.at[2]),
    ]
    for r in range(4):
        lanes = slice(r * 128, (r + 1) * 128)
        fetches.append(pltpu.make_async_copy(x_hbm.at[:, lanes], xg.at[2 + r, 0:48, :], in_sem.at[3]))
    for fetch in fetches:
        fetch.start()

    barrier = pltpu.get_barrier_semaphore()

    def greet(where):
        pl.semaphore_signal(barrier, inc=1, device_id=where, device_id_type=MESH)

    @pl.when(core == 1)
    def _():
        for o in range(1, ny):
            greet((lax.rem(ty + o, ny), tz, core, col))
        for o in range(1, nz):
            greet((ty, lax.rem(tz + o, nz), core, col))

    @pl.when(core == 0)
    def _():
        for o in range(1, nz):
            greet((ty, lax.rem(tz + o, nz), 1, col))

    for c in across_cols:
        greet(at_tile(across, c))
    greet(at_tile(after, col))
    greet(at_tile(before, col))
    for o in range(1, 4):
        greet((ty, tz, core, lax.rem(col + o, 4)))
        greet((ty, tz, 1 - core, lax.rem(col + o, 4)))
    greet((ty, tz, 1 - core, col))

    for fetch in fetches[:3]:
        fetch.wait()
    pltpu.make_async_copy(xg.at[2:6, 0:48, :], xg.at[2:6, 0:48, :], in_sem.at[3]).wait()
    lane = iota((1, 128), 1)
    rows, cols = pairs_ref[0], pairs_ref[1]
    slot_col = iota((4, 8), 0)
    counts = jnp.zeros((4, 8), jnp.int32)
    for c in range(4):
        counts = jnp.where(slot_col == c, count_ref[:, c : c + 1], counts)
    live = jnp.where(iota((4, 8), 1) < counts, 1.0, 0.0).astype(F32)
    reach = cols - t * 4 - rows
    for r in range(4):
        xg[2 + r, 48:56, :] = jnp.zeros((8, 128), F32)
        xg[2 + r, 48:51, :] = pos_ref[:, r * 128 : (r + 1) * 128]
        listed = jnp.zeros((1, 128), F32)
        for k in range(3):
            here = jnp.where((rows == r) & (reach == k), live, 0.0)
            total = jnp.sum(jnp.sum(here, axis=1, keepdims=True), axis=0, keepdims=True)
            listed = jnp.where(lane == k, total, listed)
        xg[2 + r, 51:52, :] = listed

    dacc[...] = jnp.zeros_like(dacc)
    pay[...] = jnp.zeros_like(pay)
    own = 2 + col

    def spring_block(q, slot):
        mine = [xg[own, 48 + d : 49 + d, :] for d in range(3)]
        listed = xg[jnp.minimum(slot, own), 51:52, :]
        times = jnp.sum(jnp.where(lane == jnp.abs(slot - own), listed, 0.0), axis=1, keepdims=True)
        times = times * (1.0 / 64.0)
        near = jnp.transpose(xg[slot, 48:56, :])
        sums = [dacc[m] for m in range(6)]
        for ch in range(4):
            part = near[ch * 32 : (ch + 1) * 32]
            off = [part[:, d : d + 1] - mine[d] for d in range(3)]
            dist = off[0] * off[0] + off[1] * off[1] + off[2] * off[2]
            fall = 1.0 - dist * (1.0 / 225.0)
            weight = jnp.where(dist < 225.0, fall * fall, 0.0) * times / jnp.maximum(dist, 1.0)
            by = [weight * o for o in off]
            at = pl.ds(pl.multiple_of(q * 128 + ch * 32, 32), 32)
            for m, (c, d) in enumerate(MATS):
                s = by[c] * off[d]
                hi, lo = split(s)
                shi[at, m * 128 : (m + 1) * 128] = hi
                slo[at, m * 128 : (m + 1) * 128] = lo
                sums[m] = sums[m] + ((s[0:8] + s[8:16]) + (s[16:24] + s[24:32]))
        for m in range(6):
            dacc[m] = sums[m]

    first = jnp.where(low, 2, 3)
    late = (
        jnp.where(col == 0, 0, jnp.where(col == 1, 1, jnp.where(col == 2, 2, 6))),
        jnp.where(col == 0, 1, jnp.where(col == 1, 5, jnp.where(col == 2, 6, 7))),
    )
    slots = (first, first + 1, first + 2) + late

    pl.semaphore_wait(barrier, 11 + core * (ny + 2 * nz - 3))
    from_slot, to_slot = jnp.where(low, 4, 2), jnp.where(low, 0, 6)

    def halo_copy(n, rows):
        return pltpu.make_async_remote_copy(
            src_ref=xg.at[pl.ds(from_slot, 2), rows],
            dst_ref=xg.at[pl.ds(to_slot, 2), rows],
            send_sem=halo_send.at[n],
            recv_sem=halo_recv.at[n],
            device_id=at_tile(jnp.where(low, after, before), col),
            device_id_type=MESH,
        )

    halo = (halo_copy(0, slice(48, 56)), halo_copy(1, slice(0, 48)))
    for copy in halo:
        copy.start()

    def near_vectors(source, q):
        hi, lo = split(source[slots[q], 0:48, :])
        lw[0:48, q * 128 : (q + 1) * 128] = hi
        lw[48:96, q * 128 : (q + 1) * 128] = lo

    def near_sum(start, stop):
        a, b = start * 128, stop * 128
        both = mm(lw[:, a:b], shi[a:b, :])
        return both[0:48] + both[48:96] + mm(lw[0:48, a:b], slo[a:b, :])

    def first_blocks(q, carry):
        spring_block(q, first + q)
        return carry

    lax.fori_loop(0, 3, first_blocks, 0)
    for q in range(3):
        near_vectors(xg, q)
    gathered = near_sum(0, 3)
    halo[0].wait_recv()

    def late_blocks(q, carry):
        spring_block(3 + q, jnp.where(q == 0, late[0], late[1]))
        return carry

    lax.fori_loop(0, 2, late_blocks, 0)
    halo[1].wait_recv()
    for q in range(3, 5):
        near_vectors(xg, q)
    gathered = gathered + near_sum(3, 5)
    diag = [jnp.sum(dacc[m], axis=0, keepdims=True) for m in range(6)]

    def finish_product(gathered, source):
        here = [source[own, d * 16 : (d + 1) * 16, :] for d in range(3)]
        out = []
        for c in range(3):
            acc = None
            for d in range(3):
                m = MAT_OF[(c, d)]
                term = diag[m] * here[d] - gathered[d * 16 : (d + 1) * 16, m * 128 : (m + 1) * 128]
                acc = term if acc is None else acc + term
            out.append(acc)
        return here, out

    def all_sent(buf, send):
        moved(buf, slice(None), send, q_recv, (ty, tz, 1 - core, col)).wait_send()

    def all_here(buf, recv):
        moved(buf, slice(None), q_send, recv, (ty, tz, 1 - core, col)).wait_recv()

    def moved(buf, at, send, recv, where):
        return pltpu.make_async_remote_copy(
            src_ref=buf.at[at], dst_ref=buf.at[at], send_sem=send, recv_sem=recv, device_id=where, device_id_type=MESH
        )

    here, first_product = finish_product(gathered, xg)
    for d in range(3):
        pg[own, d * 16 : (d + 1) * 16, :] = first_product[d]
    edge = jnp.logical_or(col == 0, col == 3)

    def across_copy(c):
        slot = jnp.where(low, 6 + col, col - 2)
        return pltpu.make_async_remote_copy(
            src_ref=pg.at[own], dst_ref=pg.at[slot], send_sem=p_send, recv_sem=p_recv,
            device_id=at_tile(across, c), device_id_type=MESH,
        )

    def line_copy(o, send, recv):
        return moved(pg, own, send, recv, (ty, tz, core, lax.rem(col + o, 4)))

    def rest_copy(o):
        return moved(qg, col, q_send, q_recv, (ty, tz, core, lax.rem(col + o, 4)))

    near_across = across_copy(jnp.where(low, 3, 0))
    next_across = across_copy(jnp.where(low, 2, 1))

    def is_far(o):
        return jnp.logical_and(edge, lax.rem(col + o, 4) == 3 - col)

    near_across.start()

    @pl.when(edge)
    def _():
        next_across.start()

    for o in (2, 1, 3):
        @pl.when(jnp.logical_not(is_far(o)))
        def _():
            line_copy(o, p_send, p_recv).start()

    def pay_blocks(blocks):
        for at, width, block in blocks:
            for h in range(2):
                pay[:, 64 * h + at : 64 * h + at + width] = block[8 * h : 8 * h + 8]

    x, p = jnp.concatenate(here, axis=1), jnp.concatenate(first_product, axis=1)
    z_x = mm_exact(jnp.concatenate([x, p], axis=0), x, transposed=True)
    mix = jnp.where(iota((16, 16), 1) <= iota((16, 16), 0), z_x[0:16], mm_exact(p, p, transposed=True))
    pay_blocks(((0, 16, z_x[16:32]), (32, 16, mix), (48, 1, jnp.sum(p * p, axis=1, keepdims=True))))

    all_here(pg.at[0:4], p_recv)

    for q in range(5):
        near_vectors(pg, q)
    _, second_product = finish_product(near_sum(0, 5), pg)

    for d in range(3):
        qg[col, d * 16 : (d + 1) * 16, :] = second_product[d]
    q = jnp.concatenate(second_product, axis=1)
    pay_blocks(((16, 16, mm_exact(p, q, transposed=True)), (49, 1, jnp.sum(q * q, axis=1, keepdims=True))))

    line = col * 2 + core

    def to_line(x):
        return pltpu.make_async_remote_copy(
            src_ref=pay, dst_ref=ra.at[line], send_sem=a_send, recv_sem=a_recv,
            device_id=(ty, tz, 1, x), device_id_type=MESH,
        )

    for x in range(4):
        @pl.when(jnp.logical_or(core == 0, col != x))
        def _():
            to_line(x).start()

    def y_copy(o):
        return moved(rb, ty, b_send, b_recv, (lax.rem(ty + o, ny), tz, 1, col))

    def z_copy(o, c):
        return moved(rc, tz, c_send.at[c], c_recv, (ty, lax.rem(tz + o, nz), c, col))

    def summed(buf, n):
        parts = [buf[i] for i in range(n)]
        while len(parts) > 1:
            parts = [a + b for a, b in zip(parts[0::2], parts[1::2])] + parts[len(parts) & ~1 :]
        return parts[0]

    def far_first(n):
        return sorted(range(1, n), key=lambda o: -min(o, n - o))

    products_out = (
        pltpu.make_async_copy(pg.at[2:6], pq_hbm.at[0], out_sem.at[1]),
        pltpu.make_async_copy(qg, pq_hbm.at[1], out_sem.at[2]),
    )

    def put_products():
        for o in range(1, 4):
            rest_copy(o).start()

            @pl.when(is_far(o))
            def _():
                line_copy(o, far_send, far_recv).start()

        all_here(qg.at[0:3], q_recv)

        @pl.when(edge)
        def _():
            all_here(pg.at[0], far_recv)

        for copy in products_out:
            copy.start()

    @pl.when(core == 1)
    def _():
        ra[line] = pay[...]
        all_here(ra.at[0:7], a_recv)
        rb[ty] = summed(ra, 8)
        for o in far_first(ny):
            y_copy(o).start()
        put_products()
        all_here(rb.at[0 : ny - 1], b_recv)
        rc[tz] = summed(rb, ny)
        for o in far_first(nz) + [0]:
            z_copy(o, 0).start()
            if o:
                z_copy(o, 1).start()
        all_here(rc.at[0 : nz - 1], c_recv)

    @pl.when(core == 0)
    def _():
        all_sent(ra.at[0:4], a_send)
        put_products()
        all_here(rc, c_recv)

    z_ref[...] = summed(rc, nz)
    gram_out = pltpu.make_async_copy(z_ref, z_hbm, out_sem.at[0])
    gram_out.start()

    @pl.when(core == 1)
    def _():
        all_sent(ra.at[0:3], a_send)
        all_sent(rb.at[0 : ny - 1], b_send)
        all_sent(rc, c_send.at[0])
        all_sent(rc.at[0 : nz - 1], c_send.at[1])

    all_sent(pg.at[0:4], p_send)
    all_sent(qg.at[0:3], q_send)

    @pl.when(edge)
    def _():
        all_sent(pg.at[0], far_send)

    for copy in halo:
        copy.wait_send()
    gram_out.wait()
    for copy in products_out:
        copy.wait()


def per_device(ny, nz, positions, trial_block, pair_tiles, pair_count):
    scale = 1.0 / (3.0 * ny * nz * 2 * 512)
    vmem = pl.BlockSpec(memory_space=pltpu.VMEM)
    dma = pltpu.SemaphoreType.DMA
    hbm = pl.BlockSpec(memory_space=pltpu.HBM)
    block = trial_block.reshape(48, 512)
    products, gram = pl.pallas_call(
        functools.partial(kernel, ny, nz),
        out_shape=(jax.ShapeDtypeStruct((2, 4, 48, 128), F32), jax.ShapeDtypeStruct((8, 128), F32)),
        in_specs=[hbm] * 4,
        out_specs=(hbm, hbm),
        scratch_shapes=[
            pltpu.VMEM((3, 512), F32),
            pltpu.VMEM((2, 4, 8), jnp.int32),
            pltpu.VMEM((1, 4), jnp.int32),
            dma((4,)),
            pltpu.VMEM((8, 128), F32),
            dma((3,)),
            pltpu.VMEM((8, 56, 128), F32),
            pltpu.VMEM((8, 48, 128), F32),
            pltpu.VMEM((4, 48, 128), F32),
            pltpu.VMEM((640, 768), BF16),
            pltpu.VMEM((640, 768), BF16),
            pltpu.VMEM((96, 640), BF16),
            pltpu.VMEM((6, 8, 128), F32),
            pltpu.VMEM((8, 128), F32),
            pltpu.VMEM((8, 8, 128), F32),
            pltpu.VMEM((ny, 8, 128), F32),
            pltpu.VMEM((nz, 8, 128), F32),
            dma((2,)), dma((2,)),
            dma, dma, dma, dma, dma, dma, dma, dma, dma, dma,
            dma((2,)), dma,
        ],
        compiler_params=pltpu.CompilerParams(collective_id=0, has_side_effects=True, vmem_limit_bytes=60 * 1024 * 1024),
        name="gram_blocks",
    )(block, positions, pair_tiles.reshape(2, 4, 8), pair_count)
    block, rayleigh, correlation, norms = pl.pallas_call(
        functools.partial(finish, scale),
        out_shape=(
            jax.ShapeDtypeStruct((48, 512), F32),
            jax.ShapeDtypeStruct((16, 16), F32),
            jax.ShapeDtypeStruct((16, 16), F32),
            jax.ShapeDtypeStruct((1, 16), F32),
        ),
        in_specs=[hbm] * 3,
        out_specs=(vmem,) * 4,
        scratch_shapes=[pltpu.VMEM((48, 512), F32), pltpu.VMEM((2, 4, 48, 128), F32), pltpu.VMEM((8, 128), F32), dma((3,))],
        compiler_params=pltpu.CompilerParams(vmem_limit_bytes=60 * 1024 * 1024),
        name="finish",
    )(block, products, gram)
    return block.reshape(3, 16, 512), rayleigh, correlation, norms.reshape(16)


def build(finer):
    return jax.shard_map(
        functools.partial(per_device, finer.shape["ty"], finer.shape["tz"]),
        mesh=finer,
        in_specs=(P(None, TILE), P(None, None, TILE), P(None, TILE, None, None), P(TILE, None)),
        out_specs=(P(None, None, TILE), P(), P(), P()),
        check_vma=False,
    )


def solution(mesh):
    return build(Mesh(mesh.devices.reshape(8, 8, 2, mesh.shape["col"]), (*TILE, "col")))
```
